256 devices in a mesh: member: 4 (over y, x), node: 64 (over z, core).
Axes of the slice: x: 2, y: 2, z: 32, core: 2. Of those that a mesh axis runs over, the one named last changes fastest.
The devices are a block of a 4x8x32 slice.
Arguments:
- conditioning: bfloat16 [168, 262144], P(None, ('member', 'node')), parts along dimension 1, may hold values from -6 to 6
- target_state: float32 [84, 262144], P(None, ('member', 'node')), parts along dimension 1, may hold values from -6 to 6
- noise_sample: float32 [84, 262144], P(None, ('member', 'node')), parts along dimension 1, may hold values from -6 to 6
- step_index: int32 [4], P('member'), parts along dimension 0, may hold values from 0 to 19
- mesh_features: float32 [3, 40960], P(None, 'node'), may hold values from -1 to 1
- edge_geometry: float32 [4, 262144], P(None, 'node'), may hold values from -6 to 6
- edge_slot: int32 [262144], P('node'), may hold values from 0 to 1023, as said below
- edge_receiver: int32 [262144], P('node'), may hold values from 0 to 639
- send_rows: int32 [4096, 16], P('node'), may hold values from 0 to 1023
- edge_count: int32 [64], P('node'), may hold values from 1503 to 4096, as said below
- embed_weight: bfloat16 [252, 512], replicated, may hold values from -0.375 to 0.375
- mesh_weight: float32 [3, 512], replicated, may hold values from -3.5 to 3.5
- geom_weight: float32 [4, 512], replicated, may hold values from -3 to 3
- sender_weight: bfloat16 [512, 512], P('node'), may hold values from -0.15625 to 0.15625
- edge_weight: bfloat16 [512, 512], P('node'), may hold values from -0.15625 to 0.15625
- receiver_weight: bfloat16 [512, 512], P('node'), may hold values from -0.15625 to 0.15625
- message_weight: bfloat16 [512, 512], P('node'), may hold values from -0.25 to 0.25
- node_weight: bfloat16 [1024, 512], P('node'), may hold values from -0.1875 to 0.1875
- output_weight: bfloat16 [512, 512], P('node'), may hold values from -0.25 to 0.25
- noise_weight: float32 [32, 512], replicated, may hold values from -1 to 1
- film_weight: bfloat16 [512, 2048], replicated, may hold values from -0.25 to 0.25
Outputs:
- mesh_latent: bfloat16 [40960, 2048], P('node', 'member'), parts along dimension 1
The draws below stay inside these ranges and needn't reach their ends.
There are 4 independent parts, one for each index of `member`. The reference program is written for one: setup_inputs(seed, part) draws one part's arguments, and reference() takes and returns one part's arrays. A program takes and returns all parts, laid end to end along the dimension named above; an argument that names none is the same for every part. Nothing has to cross between parts.
Inputs may be any that keep to these rules, and one draw needn't show every extreme that they name: `edge_slot`: on each device, the live slots name every entry of its 64 * 16 list at least once, or as many distinct entries as there are live slots where these are fewer. `edge_count`: the counts sum to 64 * 2048 and one device has all 4096 slots live.
All inputs are finite; a program needn't handle non-finite values.
Results may differ from the reference program's by a relative error of at most 0.0071.
Values may be sent and summed in bfloat16 or wider, within the bound.
A program may use at most 64 MiB of HBM per device.

```python
import jax
import jax.numpy as jnp
from jax import lax

LAT = 512
VARS = 84
G_DEV = 1024
M_DEV = 640
E_DEV = 4096
CAP = 16
STEPS = 20
FREQ = 16
C_COND = 168
C_RAW = 252
GRID = 65536
MESH = 40960
EDGES = 262144
PAIRS = 4096
N_NODE = 64


def live_counts(key):
    base_key = jax.random.fold_in(key, 11)
    order_key, spread_key = jax.random.split(base_key)
    order = jax.random.permutation(order_key, N_NODE).astype(jnp.int32)
    position = jnp.arange(N_NODE, dtype=jnp.int32)
    others = N_NODE - 1
    excess = E_DEV // 2
    share = excess // others
    remain = excess % others
    loss = share + (position - 1 < remain).astype(jnp.int32)
    spread = jax.random.randint(spread_key, (N_NODE,), 0, E_DEV // 8 + 1).astype(jnp.int32)
    following = jnp.where(position == N_NODE - 1, 1, position + 1).astype(jnp.int32)
    delta = spread - spread[following]
    placed = jnp.where(position == 0, E_DEV, E_DEV // 2 - loss + delta).astype(jnp.int32)
    return jnp.zeros((N_NODE,), jnp.int32).at[order].set(placed)


def draw_edge_count(key, part):
    return live_counts(key)


def draw_edge_slot(key, part):
    counts = live_counts(key)
    listed = N_NODE * CAP
    slot_key = jax.random.fold_in(key, 23)
    device_keys = jax.vmap(lambda index: jax.random.fold_in(slot_key, index))(jnp.arange(N_NODE, dtype=jnp.int32))

    def one_device(device_key, count):
        first_key, second_key = jax.random.split(device_key)
        order = jax.random.permutation(first_key, listed).astype(jnp.int32)
        extra = jax.random.randint(second_key, (E_DEV,), 0, listed).astype(jnp.int32)
        used = jnp.minimum(count, listed)
        position = jnp.arange(E_DEV, dtype=jnp.int32)
        pick = jnp.where(position < listed, position, extra % used)
        pick = jnp.minimum(pick, listed - 1)
        return order[pick]
    return jax.vmap(one_device)(device_keys, counts).reshape(N_NODE * E_DEV)


def plant(drawn, stream_key, smallest, high):
    longest = drawn.shape.index(max(drawn.shape))
    spots = []
    for shift in (0, 1):
        where = [jax.random.randint(jax.random.fold_in(stream_key, axis), (), 0, length) for axis, length in enumerate(drawn.shape)]
        where[longest] = (where[longest] + shift) % drawn.shape[longest]
        spots.append(tuple(where))
    return drawn.at[spots[0]].set(smallest).at[spots[1]].set(high)


def block_levels(key, shape, shards, least, largest):
    factor_of, own = 1.0, jax.random.fold_in(key, 6)
    for axis_at, blocks in shards:
        steps = jnp.exp(jax.random.uniform(jax.random.fold_in(own, axis_at), (blocks,), jnp.float32, least / len(shards), largest / len(shards)))
        factor_of = factor_of * jnp.repeat(steps, shape[axis_at] // blocks).reshape([-1 if axis == axis_at else 1 for axis in range(len(shape))])
    return factor_of


def gaussian(key, extent, width, limit, pieces=(), held_as=jnp.bfloat16):
    drawn = width * jax.random.normal(key, extent, jnp.float32)
    if pieces:
        drawn = drawn * block_levels(key, extent, pieces, -0.22, 0.18)
    return jnp.clip(drawn, -limit, limit).astype(held_as)


def setup_inputs(seed: int = 0, part: int = 0) -> dict:
    arg_keys = jax.random.split(jax.random.key(seed), 22)
    part_splits = jax.random.split(jax.random.fold_in(arg_keys[21], part), 22)
    return {
        "conditioning": gaussian(part_splits[0], (C_COND, GRID), 1.0, 6.0, ((1, 64),)),
        "target_state": gaussian(part_splits[1], (VARS, GRID), 1.0, 6.0, ((1, 64),), jnp.float32),
        "noise_sample": gaussian(part_splits[2], (VARS, GRID), 1.0, 6.0, ((1, 64),), jnp.float32),
        "step_index": jax.random.randint(part_splits[3], (1,), 0, STEPS).astype(jnp.int32),
        "mesh_features": jnp.clip(jax.random.uniform(arg_keys[4], (3, MESH), jnp.float32, -1.0, 1.0) * block_levels(arg_keys[4], (3, MESH), ((1, 64),), -0.4, 0.0), -1.0, 1.0),
        "edge_geometry": gaussian(arg_keys[5], (4, EDGES), 1.0, 6.0, ((1, 64),), jnp.float32),
        "edge_slot": draw_edge_slot(jax.random.fold_in(arg_keys[21], 71), part),
        "edge_receiver": plant(jax.random.randint(arg_keys[7], (EDGES,), 0, M_DEV), jax.random.fold_in(arg_keys[7], 1), 0, M_DEV - 1).astype(jnp.int32),
        "send_rows": plant(jax.random.randint(arg_keys[8], (PAIRS, CAP), 0, G_DEV), jax.random.fold_in(arg_keys[8], 1), 0, G_DEV - 1).astype(jnp.int32),
        "edge_count": draw_edge_count(jax.random.fold_in(arg_keys[21], 71), part),
        "embed_weight": gaussian(arg_keys[10], (C_RAW, LAT), C_RAW ** -0.5, 0.375),
        "mesh_weight": gaussian(arg_keys[11], (3, LAT), 3 ** -0.5, 3.5, (), jnp.float32),
        "geom_weight": gaussian(arg_keys[12], (4, LAT), 4 ** -0.5, 3.0, (), jnp.float32),
        "sender_weight": gaussian(arg_keys[13], (LAT, LAT), (3 * LAT) ** -0.5, 0.15625, ((0, 64),)),
        "edge_weight": gaussian(arg_keys[14], (LAT, LAT), (3 * LAT) ** -0.5, 0.15625, ((0, 64),)),
        "receiver_weight": gaussian(arg_keys[15], (LAT, LAT), (3 * LAT) ** -0.5, 0.15625, ((0, 64),)),
        "message_weight": gaussian(arg_keys[16], (LAT, LAT), LAT ** -0.5, 0.25, ((0, 64),)),
        "node_weight": gaussian(arg_keys[17], (2 * LAT, LAT), (2 * LAT) ** -0.5, 0.1875, ((0, 64),)),
        "output_weight": gaussian(arg_keys[18], (LAT, LAT), LAT ** -0.5, 0.25, ((0, 64),)),
        "noise_weight": gaussian(arg_keys[19], (2 * FREQ, LAT), (2 * FREQ) ** -0.5, 1.0, (), jnp.float32),
        "film_weight": gaussian(arg_keys[20], (LAT, 4 * LAT), LAT ** -0.5, 0.25),
    }


sigma_top = 80.0
sigma_low = 0.03
rho_power = 7.0
norm_eps = 1e-05

def layer_norm(values):
    mean = lax.optimization_barrier(jnp.mean(values, axis=-1, keepdims=True))
    centred = values - mean
    var = lax.optimization_barrier(jnp.mean(centred * centred, axis=-1, keepdims=True))
    return centred * lax.rsqrt(var + norm_eps)

def noise_terms(step_index, noise_weight, film_weight):
    frac = step_index[0].astype(jnp.float32) / (STEPS - 1)
    upper = sigma_top ** (1.0 / rho_power)
    lower = sigma_low ** (1.0 / rho_power)
    sigma = (upper + frac * (lower - upper)) ** rho_power
    angle = 0.25 * jnp.log(sigma) * (jnp.arange(FREQ, dtype=jnp.float32) + 1.0)
    fourier = jnp.concatenate([jnp.sin(angle), jnp.cos(angle)])[None, :]
    cond = jax.nn.silu(jnp.dot(fourier, noise_weight, precision=lax.Precision.HIGHEST)).astype(jnp.bfloat16)
    film = jnp.dot(cond, film_weight, preferred_element_type=jnp.float32)
    return (sigma, film)

def reference(conditioning, target_state, noise_sample, step_index, mesh_features, edge_geometry, edge_slot, edge_receiver, send_rows, edge_count, embed_weight, mesh_weight, geom_weight, sender_weight, edge_weight, receiver_weight, message_weight, node_weight, output_weight, noise_weight, film_weight):
    sigma, film = noise_terms(step_index, noise_weight, film_weight)
    edge_scale = film[:, 0:LAT]
    edge_shift = film[:, LAT:2 * LAT]
    node_scale = film[:, 2 * LAT:3 * LAT]
    node_shift = film[:, 3 * LAT:4 * LAT]
    noisy = ((target_state + sigma * noise_sample) / jnp.sqrt(sigma * sigma + 1.0)).astype(jnp.bfloat16)
    raw = jnp.concatenate([conditioning, noisy], axis=0)
    grid_latent = jax.nn.silu(jnp.dot(raw.T, embed_weight, preferred_element_type=jnp.float32)).astype(jnp.bfloat16)
    mesh_embed = jax.nn.silu(jnp.dot(mesh_features.T, mesh_weight, precision=lax.Precision.HIGHEST)).astype(jnp.bfloat16)
    recv_proj = jnp.dot(mesh_embed, receiver_weight, preferred_element_type=jnp.float32).astype(jnp.bfloat16)
    edge_embed = jax.nn.silu(jnp.dot(edge_geometry.T, geom_weight, precision=lax.Precision.HIGHEST)).astype(jnp.bfloat16)
    tables = send_rows.reshape(N_NODE, N_NODE, CAP)
    bands = jnp.arange(N_NODE, dtype=jnp.int32)

    def one_device(device):
        table = lax.dynamic_index_in_dim(tables, device, 1, keepdims=False)
        grid_index = (bands[:, None] * G_DEV + table).reshape(N_NODE * CAP)
        start = (device * E_DEV).astype(jnp.int32)
        slots = lax.dynamic_slice_in_dim(edge_slot, start, E_DEV, 0)
        local_recv = lax.dynamic_slice_in_dim(edge_receiver, start, E_DEV, 0)
        embed_rows = lax.dynamic_slice_in_dim(edge_embed, start, E_DEV, 0)
        node_start = (device * M_DEV).astype(jnp.int32)
        proj_local = lax.dynamic_slice_in_dim(recv_proj, node_start, M_DEV, 0)
        mesh_local = lax.dynamic_slice_in_dim(mesh_embed, node_start, M_DEV, 0)
        sender_rows = grid_latent[grid_index[slots]]
        pre = jnp.dot(embed_rows, edge_weight, preferred_element_type=jnp.float32)
        pre = pre + jnp.dot(sender_rows, sender_weight, preferred_element_type=jnp.float32)
        pre = pre + proj_local[local_recv].astype(jnp.float32)
        hidden = jax.nn.silu(pre).astype(jnp.bfloat16)
        mixed = jnp.dot(hidden, message_weight, preferred_element_type=jnp.float32)
        message = layer_norm(mixed) * (1.0 + edge_scale) + edge_shift
        count = lax.dynamic_index_in_dim(edge_count, device, 0, keepdims=False)
        live = jnp.arange(E_DEV, dtype=jnp.int32) < count
        message = jnp.where(live[:, None], message, 0.0).astype(jnp.bfloat16)
        gathered = jax.ops.segment_sum(message.astype(jnp.float32), local_recv, num_segments=M_DEV).astype(jnp.bfloat16)
        joined = jnp.concatenate([mesh_local, gathered], axis=1)
        update = jax.nn.silu(jnp.dot(joined, node_weight, preferred_element_type=jnp.float32)).astype(jnp.bfloat16)
        result = jnp.dot(update, output_weight, preferred_element_type=jnp.float32)
        return (mesh_local.astype(jnp.float32) + layer_norm(result) * (1.0 + node_scale) + node_shift).astype(jnp.bfloat16)
    blocks = lax.map(one_device, bands)
    return blocks.reshape(MESH, LAT)
```

```python
import functools

import jax
import jax.numpy as jnp
from jax import lax
from jax.experimental import pallas as pl
from jax.experimental.pallas import tpu as pltpu
from jax.sharding import PartitionSpec as P

STEPS = 20
sigma_top = 80.0
sigma_low = 0.03
rho_power = 7.0
norm_eps = 1e-05
MESH = pl.DeviceIdType.MESH
VMEM = pl.BlockSpec(memory_space=pltpu.VMEM)
SMEM = pl.BlockSpec(memory_space=pltpu.SMEM)
ANY = pl.BlockSpec(memory_space=pl.ANY)
LIMIT = 60 * 1024 * 1024
f32, bf16 = jnp.float32, jnp.bfloat16


def silu(x):
    half = 0.5 * x
    return half + half * jnp.tanh(half)


def turned(x):
    return x.astype(f32).T


def pick_kernel(scal, cond, target, noise, rows, out, raw):
    chans, points = raw.shape
    vars_ = target.shape[0]
    lead = chans - cond.shape[0]
    noisy = (target[...] + scal[0] * noise[...]) / scal[1]
    raw[0:vars_] = noisy
    if lead > vars_:
        raw[vars_:lead] = jnp.zeros((lead - vars_, points), f32)
    raw[lead:chans] = cond[...].astype(f32)
    picks = rows.shape[1]
    values = raw[...].astype(bf16)
    ids = lax.broadcasted_iota(jnp.int32, (points, picks), 0)
    one_hot = jnp.where(ids == rows[...], 1.0, 0.0).astype(bf16)
    out[...] = jnp.dot(values, one_hot, preferred_element_type=f32).T.astype(bf16)


def exchange_kernel(
    devices, x, wa, wb, wc, wd, wo, wn, o, w_all, w_node,
    local, ready_r, ready_l, pair, send, recv, ring_s, ring_r, part_s, part_r,
):
    chips = devices // 2
    half = chips // 2
    me = lax.axis_index("node")
    z, c = me // 2, lax.rem(me, 2)
    right, left = lax.rem(me + 2, devices), lax.rem(me + devices - 2, devices)
    part = z * 2 + 1 - c
    barrier = pltpu.get_barrier_semaphore()
    for t in (right, left, part):
        pl.semaphore_signal(barrier, inc=1, device_id={"node": t}, device_id_type=MESH)
    rows = wa.shape[0]
    width = wa.shape[1]
    node_rows = wn.shape[0]
    cap = x.shape[0] // devices

    def place(n):
        return w_all.at[pl.ds(pl.multiple_of(n * rows, rows), rows)]

    def place_node(n):
        return w_node.at[pl.ds(pl.multiple_of(n * node_rows, node_rows), node_rows)]

    own = [
        pltpu.make_async_copy(w, place(me).at[:, width * k : width * (k + 1)], local.at[k])
        for k, w in enumerate((wa, wb, wc, wd, wo))
    ]
    own.append(pltpu.make_async_copy(wn, place_node(me), local.at[5]))

    def block(ref, n):
        return ref.at[pl.ds(pl.multiple_of(n * cap, cap), cap)]

    own.append(pltpu.make_async_copy(block(x, me), block(o, me), local.at[6]))
    for copy in own:
        copy.start()
    for copy in own:
        copy.wait()
    pl.semaphore_wait(barrier, 3)
    pl.semaphore_signal(pair, inc=1, device_id={"node": part}, device_id_type=MESH)

    def ring(direction, n, s, target):
        return [
            pltpu.make_async_remote_copy(
                src_ref=ref(n), dst_ref=ref(n),
                send_sem=ring_s.at[direction, k, s], recv_sem=ring_r.at[direction, k, s],
                device_id={"node": target}, device_id_type=MESH,
            )
            for k, ref in enumerate((place, place_node))
        ]

    def to_part(i, n):
        return [
            pltpu.make_async_remote_copy(
                src_ref=ref(n), dst_ref=ref(n),
                send_sem=part_s.at[k, i], recv_sem=part_r.at[k, i],
                device_id={"node": part}, device_id_type=MESH,
            )
            for k, ref in enumerate((place, place_node))
        ]

    def points(i, target):
        return pltpu.make_async_remote_copy(
            src_ref=block(x, target), dst_ref=block(o, me),
            send_sem=send.at[i], recv_sem=recv.at[i],
            device_id={"node": target}, device_id_type=MESH,
        )

    def start(copies):
        for copy in copies:
            copy.start()

    start(ring(0, me, 0, right))
    start(ring(1, me, 0, left))
    pl.semaphore_wait(pair, 1)
    points(0, part).start()
    start(to_part(0, me))

    def chip(k):
        return lax.rem(z + k + 2 * chips, chips)

    def announce(k):
        @pl.when(k < half)
        def _():
            pl.semaphore_signal(ready_r.at[k + 1], inc=1, device_id={"node": left}, device_id_type=MESH)

        @pl.when(k < half - 1)
        def _():
            pl.semaphore_signal(ready_l.at[k + 1], inc=1, device_id={"node": right}, device_id_type=MESH)

    def offer(k):
        @pl.when(k > 1)
        def _():
            pl.semaphore_wait(ready_r.at[k], 1)

            @pl.when(k < half)
            def _():
                pl.semaphore_wait(ready_l.at[k], 1)

        announce(k)
        for other in (0, 1):
            points(k * 4 + other, chip(k) * 2 + lax.rem(c + other, 2)).start()

            @pl.when(k < half)
            def _():
                points(k * 4 + 2 + other, chip(-k) * 2 + lax.rem(c + other, 2)).start()

    def step(k, carry):
        n = chip(-k) * 2 + c
        for copy in ring(0, n, k - 1, right):
            copy.wait_recv()

        @pl.when(k < half)
        def _():
            start(ring(0, n, k, right))

        start(to_part(k, n))

        @pl.when(k < half)
        def _():
            m = chip(k) * 2 + c
            for copy in ring(1, m, k - 1, left):
                copy.wait_recv()

            @pl.when(k < half - 1)
            def _():
                start(ring(1, m, k, left))

            start(to_part(half + k, m))

        offer(k)
        return carry

    lax.fori_loop(1, half + 1, step, 0)

    def drain(k, carry):
        for copy in to_part(k, me):
            copy.wait()

        @pl.when(k < half)
        def _():
            for copy in ring(0, me, k, right):
                copy.wait_send()

        @pl.when(k < half - 1)
        def _():
            for copy in ring(1, me, k, left):
                copy.wait_send()

        return carry

    lax.fori_loop(0, chips, drain, 0)

    def arrive(k, carry):
        for j in range(2):
            points(k * 4 + j, part).wait()

            @pl.when(k < half)
            def _():
                points(k * 4 + 2 + j, part).wait()

        return carry

    points(0, part).wait()
    lax.fori_loop(1, half + 1, arrive, 0)


def edge_kernel(
    first, count, fourier, arrived, w_all, w_node, embed, mesh_features, mesh_weight, geometry, geom_weight,
    slots, receivers, noise_weight, film_weight, out,
    emb, small, left, right, msg_t, node_t, out_t, geom_b, film_b, joined, total,
):
    width = embed.shape[1]
    mesh_count = mesh_features.shape[1]
    listed = arrived.shape[0]
    chans = arrived.shape[1]
    block = right.shape[1]
    blocks = slots.shape[1] // block
    k_mesh, k_geom = mesh_weight.shape[0], geom_weight.shape[0]
    base_s = mesh_count
    base_e = mesh_count + listed

    def weight(k):
        return w_all[:, width * k : width * (k + 1)]

    left[:, base_e : base_e + width] = turned(weight(1)).astype(bf16)
    msg_t[...] = turned(weight(3)).astype(bf16)
    out_t[...] = turned(weight(4)).astype(bf16)
    node_t[...] = turned(w_node[...]).astype(bf16)
    cond = silu(jnp.sum(fourier[...] * noise_weight[...], axis=0, keepdims=True)).astype(bf16)
    cond = jnp.broadcast_to(cond.astype(f32), (8, width)).astype(bf16)
    for k in range(4):
        piece = jnp.dot(cond, film_weight[:, width * k : width * (k + 1)], preferred_element_type=f32)
        column = piece.T[:, 0:1]
        if k % 2 == 0:
            column = column + 1.0
        film_b[k] = jnp.broadcast_to(column, (width, 128))
    small[0:k_mesh] = mesh_weight[...]
    small[k_mesh : k_mesh + k_geom] = geom_weight[...]
    small[k_mesh + k_geom : 8] = jnp.zeros((8 - k_mesh - k_geom, width), f32)
    small_t = small[...].T
    pre = small_t[:, 0:1] * mesh_features[0:1, :]
    for k in range(1, k_mesh):
        pre = pre + small_t[:, k : k + 1] * mesh_features[k : k + 1, :]
    joined[0:width] = silu(pre).astype(bf16)
    recv_t = turned(weight(2)).astype(bf16)
    left[:, 0:mesh_count] = jnp.dot(recv_t, joined[0:width], preferred_element_type=f32).astype(bf16)
    for k in range(k_geom):
        geom_b[k] = jnp.broadcast_to(small_t[:, k_mesh + k : k_mesh + k + 1], (width, 128))
    rest = embed.shape[0] - first
    lead = chans - first
    emb[0:rest] = embed[first:, :].astype(f32)
    if lead > rest:
        emb[rest:lead] = jnp.zeros((lead - rest, width), f32)
    emb[lead:chans] = embed[0:first, :].astype(f32)
    emb_t = emb[...].T.astype(bf16)
    latent = silu(
        lax.dot_general(emb_t, arrived[...], (((1,), (1,)), ((), ())), preferred_element_type=f32)
    ).astype(bf16)
    send_t = turned(weight(0)).astype(bf16)
    left[:, base_s : base_s + listed] = jnp.dot(send_t, latent, preferred_element_type=f32).astype(bf16)
    total[...] = jnp.zeros_like(total)

    def add_block(b, carry):
        start = pl.multiple_of(b * block, block)
        lanes = lax.broadcasted_iota(jnp.int32, (1, block), 1) + start
        local = jnp.where(lanes < count[0], receivers[:, pl.ds(start, block)], -1)
        ids = lax.broadcasted_iota(jnp.int32, (mesh_count, block), 0)
        right[0:mesh_count] = jnp.where(ids == local, 1.0, 0.0).astype(bf16)
        ids = lax.broadcasted_iota(jnp.int32, (listed, block), 0)
        right[base_s : base_s + listed] = jnp.where(ids == slots[:, pl.ds(start, block)], 1.0, 0.0).astype(bf16)
        for j in range(block // 128):
            geo = geometry[:, pl.ds(pl.multiple_of(start + 128 * j, 128), 128)]
            pre = geom_b[0] * geo[0:1]
            for k in range(1, k_geom):
                pre = pre + geom_b[k] * geo[k : k + 1]
            right[base_e : base_e + width, 128 * j : 128 * (j + 1)] = silu(pre).astype(bf16)
        pre = jnp.dot(left[...], right[...], preferred_element_type=f32)
        hidden = silu(pre).astype(bf16)
        mixed = jnp.dot(msg_t[...], hidden, preferred_element_type=f32)
        mean = jnp.mean(mixed, axis=0, keepdims=True)
        centred = mixed - mean
        var = jnp.mean(centred * centred, axis=0, keepdims=True)
        normed = centred * lax.rsqrt(var + norm_eps)
        pieces = [
            (normed[:, 128 * j : 128 * (j + 1)] * film_b[0] + film_b[1]).astype(bf16)
            for j in range(block // 128)
        ]
        message = jnp.concatenate(pieces, axis=1)
        total[...] += lax.dot_general(
            message, right[0:mesh_count], (((1,), (1,)), ((), ())), preferred_element_type=f32
        )
        return carry

    lax.fori_loop(0, blocks, add_block, 0)
    joined[width : 2 * width] = total[...].astype(bf16)
    update = silu(jnp.dot(node_t[...], joined[...], preferred_element_type=f32)).astype(bf16)
    result = jnp.dot(out_t[...], update, preferred_element_type=f32)
    mean = jnp.mean(result, axis=0, keepdims=True)
    centred = result - mean
    var = jnp.mean(centred * centred, axis=0, keepdims=True)
    normed = centred * lax.rsqrt(var + norm_eps)
    for j in range(mesh_count // 128):
        at = slice(128 * j, 128 * (j + 1))
        piece = joined[0:width, at].astype(f32) + normed[:, at] * film_b[2] + film_b[3]
        out[at, :] = piece.T.astype(bf16)


def per_device(
    devices, conditioning, target_state, noise_sample, step_index, mesh_features, edge_geometry,
    edge_slot, edge_receiver, send_rows, edge_count, embed_weight, mesh_weight, geom_weight,
    sender_weight, edge_weight, receiver_weight, message_weight, node_weight, output_weight,
    noise_weight, film_weight,
):
    width = embed_weight.shape[1]
    freqs = noise_weight.shape[0] // 2
    frac = step_index[0].astype(f32) / (STEPS - 1)
    upper = sigma_top ** (1.0 / rho_power)
    lower = sigma_low ** (1.0 / rho_power)
    sigma = (upper + frac * (lower - upper)) ** rho_power
    angle = 0.25 * jnp.log(sigma) * (jnp.arange(freqs, dtype=f32) + 1.0)
    fourier = jnp.concatenate([jnp.sin(angle), jnp.cos(angle)])[:, None]
    scal = jnp.stack([sigma, jnp.sqrt(sigma * sigma + 1.0)])
    points = conditioning.shape[1]
    chans = (conditioning.shape[0] + target_state.shape[0] + 7) // 8 * 8
    picks = send_rows.size
    params = functools.partial(pltpu.CompilerParams, vmem_limit_bytes=LIMIT)
    outgoing = pl.pallas_call(
        pick_kernel,
        out_shape=jax.ShapeDtypeStruct((picks, chans), bf16),
        in_specs=[SMEM, VMEM, VMEM, VMEM, VMEM],
        out_specs=VMEM,
        scratch_shapes=[pltpu.VMEM((chans, points), f32)],
        compiler_params=params(),
        name="pick",
    )(scal, conditioning, target_state, noise_sample, send_rows.reshape(1, picks))
    half = devices // 4
    sem = pltpu.SemaphoreType
    arrived, w_all, w_node = pl.pallas_call(
        functools.partial(exchange_kernel, devices),
        out_shape=(
            jax.ShapeDtypeStruct((picks, chans), bf16),
            jax.ShapeDtypeStruct((devices * sender_weight.shape[0], 5 * width), bf16),
            jax.ShapeDtypeStruct((devices * node_weight.shape[0], width), bf16),
        ),
        in_specs=[VMEM] + [ANY] * 6,
        out_specs=(VMEM, VMEM, VMEM),
        scratch_shapes=[
            sem.DMA((7,)),
            sem.REGULAR((half + 1,)),
            sem.REGULAR((half + 1,)),
            sem.REGULAR,
            sem.DMA((4 * half + 4,)),
            sem.DMA((4 * half + 4,)),
            sem.DMA((2, 2, half)),
            sem.DMA((2, 2, half)),
            sem.DMA((2, 2 * half)),
            sem.DMA((2, 2 * half)),
        ],
        compiler_params=params(collective_id=0, has_side_effects=True),
        name="exchange",
    )(outgoing, sender_weight, edge_weight, receiver_weight, message_weight, output_weight, node_weight)
    slots_n = edge_slot.shape[0]
    mesh_count = mesh_features.shape[1]
    block = min(512, slots_n)
    deep = mesh_count + picks + width
    return pl.pallas_call(
        functools.partial(edge_kernel, conditioning.shape[0]),
        out_shape=jax.ShapeDtypeStruct((mesh_count, width), bf16),
        in_specs=[SMEM] + [VMEM] * 13,
        out_specs=VMEM,
        scratch_shapes=[
            pltpu.VMEM((chans, width), f32),
            pltpu.VMEM((8, width), f32),
            pltpu.VMEM((width, deep), bf16),
            pltpu.VMEM((deep, block), bf16),
            pltpu.VMEM((width, width), bf16),
            pltpu.VMEM((width, 2 * width), bf16),
            pltpu.VMEM((width, width), bf16),
            pltpu.VMEM((geom_weight.shape[0], width, 128), f32),
            pltpu.VMEM((4, width, 128), f32),
            pltpu.VMEM((2 * width, mesh_count), bf16),
            pltpu.VMEM((width, mesh_count), f32),
        ],
        compiler_params=params(),
        name="edges",
    )(
        edge_count, fourier, arrived, w_all, w_node, embed_weight, mesh_features, mesh_weight,
        edge_geometry, geom_weight, edge_slot.reshape(1, slots_n), edge_receiver.reshape(1, slots_n),
        noise_weight, film_weight,
    )


def solution(mesh):
    both = P(None, ("member", "node"))
    placed = (
        both, both, both, P("member"), P(None, "node"), P(None, "node"), P("node"), P("node"),
        P("node", None), P("node"), P(), P(), P(), P("node", None), P("node", None), P("node", None),
        P("node", None), P("node", None), P("node", None), P(), P(),
    )
    return jax.shard_map(
        functools.partial(per_device, mesh.shape["node"]),
        mesh=mesh, in_specs=placed, out_specs=P("node", "member"), check_vma=False,
    )
```

```python
import functools

import jax
import jax.numpy as jnp
from jax import lax
from jax.experimental import pallas as pl
from jax.experimental.pallas import tpu as pltpu
from jax.sharding import PartitionSpec as P

STEPS = 20
sigma_top = 80.0
sigma_low = 0.03
rho_power = 7.0
norm_eps = 1e-05
MESH = pl.DeviceIdType.MESH
VMEM = pl.BlockSpec(memory_space=pltpu.VMEM)
SMEM = pl.BlockSpec(memory_space=pltpu.SMEM)
ANY = pl.BlockSpec(memory_space=pl.ANY)
LIMIT = 60 * 1024 * 1024
f32, bf16 = jnp.float32, jnp.bfloat16


def silu(x):
    half = 0.5 * x
    return half + half * jnp.tanh(half)


def turned(x):
    return x.astype(f32).T


def exchange_kernel(
    devices, step_index, cond, target, noise, table, wa, wb, wc, wd, wo, wn, o, w_all, w_node,
    raw, x, local, ready_r, ready_l, pair, send, recv, long_s, long_r, near_s, near_r, side_s, side_r,
    part_s, part_r,
):
    chips = devices // 2
    half = chips // 2
    me = lax.axis_index("node")
    z, c = me // 2, lax.rem(me, 2)
    group = lax.axis_index("member")
    lane = lax.rem(group, 4)
    first = group - lane
    sides = [first + lax.rem(lane + k, 2) + 2 * lax.rem(lane // 2 + k // 2, 2) for k in (1, 2)]
    sides.append(first + lax.rem(lane + 1, 2) + 2 * lax.rem(lane // 2 + 1, 2))

    def chip(k):
        return lax.rem(z + k + 2 * chips, chips)

    def at(k):
        return {"node": chip(k) * 2 + c}

    part = {"node": z * 2 + 1 - c}
    right, left, far_r, far_l = at(1), at(-1), at(4), at(-4)
    barrier = pltpu.get_barrier_semaphore()
    greeted = [right, left, far_r, far_l, part] + [{"member": s} for s in sides]
    for t in greeted:
        pl.semaphore_signal(barrier, inc=1, device_id=t, device_id_type=MESH)
    rows, width = wa.shape
    node_rows = wn.shape[0]
    picks = x.shape[0]
    cap = picks // devices
    wide = w_all.shape[3] // 4
    node_wide = w_node.shape[3] // 4
    own = [
        pltpu.make_async_copy(w, w_all.at[z, c, :, width * k : width * (k + 1)], local.at[k])
        for k, w in enumerate((wa, wb, wc, wd, wo))
    ]
    own.append(pltpu.make_async_copy(wn, w_node.at[z, c], local.at[5]))
    for copy in own:
        copy.start()
    for copy in own:
        copy.wait()
    refs = (
        lambda n: w_all.at[n, c, :, pl.ds(pl.multiple_of(lane * wide, 128), wide)],
        lambda n: w_node.at[n, c, :, pl.ds(pl.multiple_of(lane * node_wide, 128), node_wide)],
    )

    def piece(n, target, s, r):
        return [
            pltpu.make_async_remote_copy(
                src_ref=ref(n), dst_ref=ref(n), send_sem=s(k), recv_sem=r(k),
                device_id=target, device_id_type=MESH,
            )
            for k, ref in enumerate(refs)
        ]

    def start(copies):
        for copy in copies:
            copy.start()

    def landed(copies):
        for copy in copies:
            copy.wait_recv()

    def long_hop(e, n, target):
        return piece(n, target, lambda k: long_s.at[k, e], lambda k: long_r.at[k, e])

    def near(kind, e, n):
        target = left if kind == 2 else right
        return piece(n, target, lambda k: near_s.at[kind, k, e], lambda k: near_r.at[kind, k, e])

    def aside(n):
        for p, s in enumerate(sides):
            start(piece(n, {"member": s}, lambda k: side_s.at[p, k], lambda k: side_r.at[p, k]))

    def spread(e, n):
        start(near(0, e, n))
        start(near(2, e, n))

    pl.semaphore_wait(barrier, len(greeted))
    pl.semaphore_signal(pair, inc=1, device_id=part, device_id_type=MESH)
    start(long_hop(1, z, far_r))
    start(long_hop(5, z, far_l))
    spread(0, z)

    vars_ = target.shape[0]
    chans, points_n = raw.shape
    lead = chans - cond.shape[0]
    frac = jnp.full((1, 128), step_index[0], jnp.int32).astype(f32) / (STEPS - 1)
    upper = sigma_top ** (1.0 / rho_power)
    lower = sigma_low ** (1.0 / rho_power)
    base = upper + frac * (lower - upper)
    square = base * base
    sigma = square * square * square * base
    scale = jnp.sqrt(sigma * sigma + 1.0)
    for j in range(points_n // 128):
        lanes = slice(128 * j, 128 * (j + 1))
        raw[0:vars_, lanes] = (target[:, lanes] + sigma * noise[:, lanes]) / scale
    if lead > vars_:
        raw[vars_:lead] = jnp.zeros((lead - vars_, points_n), f32)
    raw[lead:chans] = cond[...].astype(f32)
    spot = lax.broadcasted_iota(jnp.int32, (cap, picks), 1)
    expand = (lax.rem(spot, cap) == lax.broadcasted_iota(jnp.int32, (cap, picks), 0)).astype(f32)
    entries = table[...]
    high, low = entries // 32, lax.rem(entries, 32)
    parts = [
        jnp.dot(part_.astype(f32).astype(bf16), expand.astype(bf16), preferred_element_type=f32)
        for part_ in (high, low)
    ]
    full = parts[0] * 32.0 + parts[1]
    spot = lax.broadcasted_iota(jnp.int32, (devices, picks), 1)
    mine = spot // cap == lax.broadcasted_iota(jnp.int32, (devices, picks), 0)
    wanted = jnp.sum(jnp.where(mine, full, 0.0), axis=0, keepdims=True).astype(jnp.int32)
    values = raw[...].astype(bf16)
    ids = lax.broadcasted_iota(jnp.int32, (points_n, picks), 0)
    one_hot = jnp.where(ids == wanted, 1.0, 0.0).astype(bf16)
    x[...] = jnp.dot(values, one_hot, preferred_element_type=f32).T.astype(bf16)

    def block(ref, n):
        return ref.at[pl.ds(pl.multiple_of(n * cap, cap), cap)]

    o[pl.ds(pl.multiple_of(me * cap, cap), cap)] = x[pl.ds(pl.multiple_of(me * cap, cap), cap)]

    def points(i, n):
        return pltpu.make_async_remote_copy(
            src_ref=block(x, n), dst_ref=block(o, me), send_sem=send.at[i], recv_sem=recv.at[i],
            device_id={"node": n}, device_id_type=MESH,
        )

    def offer(k):
        for other in (0, 1):
            points(k * 4 + other, chip(k) * 2 + lax.rem(c + other, 2)).start()

            @pl.when(k < half)
            def _():
                points(k * 4 + 2 + other, chip(-k) * 2 + lax.rem(c + other, 2)).start()

    def announce(k):
        @pl.when(k < half)
        def _():
            pl.semaphore_signal(ready_r.at[k + 1], inc=1, device_id=left, device_id_type=MESH)

        @pl.when(k < half - 1)
        def _():
            pl.semaphore_signal(ready_l.at[k + 1], inc=1, device_id=right, device_id_type=MESH)

    def hear(k):
        pl.semaphore_wait(ready_r.at[k], 1)

        @pl.when(k < half)
        def _():
            pl.semaphore_wait(ready_l.at[k], 1)

    pl.semaphore_wait(pair, 1)
    announce(1)
    points(0, z * 2 + 1 - c).start()
    offer(1)
    reach = chips // 8

    def rounds(j, carry):
        @pl.when(j <= reach)
        def _():
            n = chip(-4 * j)
            landed(long_hop(j, n, far_r))

            @pl.when(j < reach)
            def _():
                start(long_hop(j + 1, n, far_r))

            spread(j, n)
            aside(n)

        @pl.when(j < reach)
        def _():
            n = chip(4 * j)
            landed(long_hop(4 + j, n, far_l))

            @pl.when(j < reach - 1)
            def _():
                start(long_hop(5 + j, n, far_l))

            spread(4 + j, n)
            aside(n)

        def from_near(e, shift):
            n = chip(shift - 1)
            landed(near(0, e, n))
            start(near(1, e, n))
            aside(n)
            m = chip(shift + 1)
            landed(near(2, e, m))
            aside(m)

        def from_two(e, shift):
            n = chip(shift - 2)
            landed(near(1, e, n))
            aside(n)

        for t in range(4):
            k = 4 * j - 2 + t

            @pl.when(k <= half)
            def _():
                hear(k)
                announce(k)
                offer(k)

        i = j - 1

        @pl.when(i <= reach)
        def _():
            from_near(i, -4 * i)

        @pl.when((i >= 1) & (i < reach))
        def _():
            from_near(4 + i, 4 * i)

        h = j - 2

        @pl.when(h >= 0)
        def _():
            from_two(h, -4 * h)

        @pl.when((h >= 1) & (h < reach))
        def _():
            from_two(4 + h, 4 * h)

        return carry

    lax.fori_loop(1, reach + 3, rounds, 0)

    def quarter(q):
        return (
            w_all.at[0 : chips - 1, c, :, wide * q : wide * (q + 1)],
            w_node.at[0 : chips - 1, c, :, node_wide * q : node_wide * (q + 1)],
        )

    def side_all(p):
        return [
            pltpu.make_async_remote_copy(
                src_ref=ref, dst_ref=ref, send_sem=side_s.at[p, k], recv_sem=side_r.at[p, k],
                device_id={"member": sides[p]}, device_id_type=MESH,
            )
            for k, ref in enumerate(quarter(0))
        ]

    for p in range(3):
        landed(side_all(p))
    over = [
        pltpu.make_async_remote_copy(
            src_ref=ref.at[:, c], dst_ref=ref.at[:, c], send_sem=part_s.at[k], recv_sem=part_r.at[k],
            device_id=part, device_id_type=MESH,
        )
        for k, ref in enumerate((w_all, w_node))
    ]
    start(over)
    for p in range(3):
        for copy in side_all(p):
            copy.wait_send()

    def sent(e, carry):
        @pl.when(e > 0)
        def _():
            for copy in long_hop(e, z, far_r):
                copy.wait_send()

        for kind in range(3):
            for copy in near(kind, e, z):
                copy.wait_send()

        return carry

    lax.fori_loop(0, 2 * reach, sent, 0)

    def arrive(k, carry):
        for j in range(2):
            points(k * 4 + j, me).wait()

            @pl.when(k < half)
            def _():
                points(k * 4 + 2 + j, me).wait()

        return carry

    points(0, me).wait()
    lax.fori_loop(1, half + 1, arrive, 0)
    for copy in over:
        copy.wait()


def edge_kernel(
    first, count, fourier, arrived, w_all, w_node, embed, mesh_features, mesh_weight, geometry, geom_weight,
    slots, receivers, noise_weight, film_weight, out,
    emb, small, left, right, msg_t, node_t, out_t, geom_b, film_b, joined, total,
):
    width = embed.shape[1]
    mesh_count = mesh_features.shape[1]
    listed = arrived.shape[0]
    chans = arrived.shape[1]
    block = right.shape[1]
    blocks = slots.shape[1] // block
    k_mesh, k_geom = mesh_weight.shape[0], geom_weight.shape[0]
    base_s = mesh_count
    base_e = mesh_count + listed

    def weight(k):
        return w_all[:, width * k : width * (k + 1)]

    left[:, base_e : base_e + width] = turned(weight(1)).astype(bf16)
    msg_t[...] = turned(weight(3)).astype(bf16)
    out_t[...] = turned(weight(4)).astype(bf16)
    node_t[...] = turned(w_node[...]).astype(bf16)
    cond = silu(jnp.sum(fourier[...] * noise_weight[...], axis=0, keepdims=True)).astype(bf16)
    cond = jnp.broadcast_to(cond.astype(f32), (8, width)).astype(bf16)
    for k in range(4):
        piece = jnp.dot(cond, film_weight[:, width * k : width * (k + 1)], preferred_element_type=f32)
        column = piece.T[:, 0:1]
        if k % 2 == 0:
            column = column + 1.0
        film_b[k] = jnp.broadcast_to(column, (width, 128))
    small[0:k_mesh] = mesh_weight[...]
    small[k_mesh : k_mesh + k_geom] = geom_weight[...]
    small[k_mesh + k_geom : 8] = jnp.zeros((8 - k_mesh - k_geom, width), f32)
    small_t = small[...].T
    pre = small_t[:, 0:1] * mesh_features[0:1, :]
    for k in range(1, k_mesh):
        pre = pre + small_t[:, k : k + 1] * mesh_features[k : k + 1, :]
    joined[0:width] = silu(pre).astype(bf16)
    recv_t = turned(weight(2)).astype(bf16)
    left[:, 0:mesh_count] = jnp.dot(recv_t, joined[0:width], preferred_element_type=f32).astype(bf16)
    for k in range(k_geom):
        geom_b[k] = jnp.broadcast_to(small_t[:, k_mesh + k : k_mesh + k + 1], (width, 128))
    rest = embed.shape[0] - first
    lead = chans - first
    emb[0:rest] = embed[first:, :].astype(f32)
    if lead > rest:
        emb[rest:lead] = jnp.zeros((lead - rest, width), f32)
    emb[lead:chans] = embed[0:first, :].astype(f32)
    emb_t = emb[...].T.astype(bf16)
    latent = silu(
        lax.dot_general(emb_t, arrived[...], (((1,), (1,)), ((), ())), preferred_element_type=f32)
    ).astype(bf16)
    send_t = turned(weight(0)).astype(bf16)
    left[:, base_s : base_s + listed] = jnp.dot(send_t, latent, preferred_element_type=f32).astype(bf16)
    total[...] = jnp.zeros_like(total)

    def add_block(b, carry):
        start = pl.multiple_of(b * block, block)
        lanes = lax.broadcasted_iota(jnp.int32, (1, block), 1) + start
        local = jnp.where(lanes < count[0], receivers[:, pl.ds(start, block)], -1)
        ids = lax.broadcasted_iota(jnp.int32, (mesh_count, block), 0)
        right[0:mesh_count] = jnp.where(ids == local, 1.0, 0.0).astype(bf16)
        ids = lax.broadcasted_iota(jnp.int32, (listed, block), 0)
        right[base_s : base_s + listed] = jnp.where(ids == slots[:, pl.ds(start, block)], 1.0, 0.0).astype(bf16)
        for j in range(block // 128):
            geo = geometry[:, pl.ds(pl.multiple_of(start + 128 * j, 128), 128)]
            pre = geom_b[0] * geo[0:1]
            for k in range(1, k_geom):
                pre = pre + geom_b[k] * geo[k : k + 1]
            right[base_e : base_e + width, 128 * j : 128 * (j + 1)] = silu(pre).astype(bf16)
        pre = jnp.dot(left[...], right[...], preferred_element_type=f32)
        hidden = silu(pre).astype(bf16)
        mixed = jnp.dot(msg_t[...], hidden, preferred_element_type=f32)
        mean = jnp.mean(mixed, axis=0, keepdims=True)
        centred = mixed - mean
        var = jnp.mean(centred * centred, axis=0, keepdims=True)
        normed = centred * lax.rsqrt(var + norm_eps)
        pieces = [
            (normed[:, 128 * j : 128 * (j + 1)] * film_b[0] + film_b[1]).astype(bf16)
            for j in range(block // 128)
        ]
        message = jnp.concatenate(pieces, axis=1)
        total[...] += lax.dot_general(
            message, right[0:mesh_count], (((1,), (1,)), ((), ())), preferred_element_type=f32
        )
        return carry

    lax.fori_loop(0, blocks, add_block, 0)
    joined[width : 2 * width] = total[...].astype(bf16)
    update = silu(jnp.dot(node_t[...], joined[...], preferred_element_type=f32)).astype(bf16)
    result = jnp.dot(out_t[...], update, preferred_element_type=f32)
    mean = jnp.mean(result, axis=0, keepdims=True)
    centred = result - mean
    var = jnp.mean(centred * centred, axis=0, keepdims=True)
    normed = centred * lax.rsqrt(var + norm_eps)
    for j in range(mesh_count // 128):
        at = slice(128 * j, 128 * (j + 1))
        piece = joined[0:width, at].astype(f32) + normed[:, at] * film_b[2] + film_b[3]
        out[at, :] = piece.T.astype(bf16)


def per_device(
    devices, conditioning, target_state, noise_sample, step_index, mesh_features, edge_geometry,
    edge_slot, edge_receiver, send_rows, edge_count, embed_weight, mesh_weight, geom_weight,
    sender_weight, edge_weight, receiver_weight, message_weight, node_weight, output_weight,
    noise_weight, film_weight,
):
    width = embed_weight.shape[1]
    freqs = noise_weight.shape[0] // 2
    frac = step_index[0].astype(f32) / (STEPS - 1)
    upper = sigma_top ** (1.0 / rho_power)
    lower = sigma_low ** (1.0 / rho_power)
    sigma = (upper + frac * (lower - upper)) ** rho_power
    angle = 0.25 * jnp.log(sigma) * (jnp.arange(freqs, dtype=f32) + 1.0)
    fourier = jnp.concatenate([jnp.sin(angle), jnp.cos(angle)])[:, None]
    points = conditioning.shape[1]
    chans = (conditioning.shape[0] + target_state.shape[0] + 7) // 8 * 8
    picks = send_rows.size
    params = functools.partial(pltpu.CompilerParams, vmem_limit_bytes=LIMIT)
    chips = devices // 2
    half = chips // 2
    sem = pltpu.SemaphoreType
    rows, node_rows = sender_weight.shape[0], node_weight.shape[0]
    arrived, w_all, w_node = pl.pallas_call(
        functools.partial(exchange_kernel, devices),
        out_shape=(
            jax.ShapeDtypeStruct((picks, chans), bf16),
            jax.ShapeDtypeStruct((chips, 2, rows, 5 * width), bf16),
            jax.ShapeDtypeStruct((chips, 2, node_rows, width), bf16),
        ),
        in_specs=[SMEM] + [VMEM] * 4 + [ANY] * 6,
        out_specs=(VMEM, VMEM, VMEM),
        scratch_shapes=[
            pltpu.VMEM((chans, points), f32),
            pltpu.VMEM((picks, chans), bf16),
            sem.DMA((6,)),
            sem.REGULAR((half + 1,)),
            sem.REGULAR((half + 1,)),
            sem.REGULAR,
            sem.DMA((4 * half + 4,)),
            sem.DMA((4 * half + 4,)),
            sem.DMA((2, chips // 4)),
            sem.DMA((2, chips // 4)),
            sem.DMA((3, 2, chips // 4)),
            sem.DMA((3, 2, chips // 4)),
            sem.DMA((3, 2)),
            sem.DMA((3, 2)),
            sem.DMA((2,)),
            sem.DMA((2,)),
        ],
        compiler_params=params(collective_id=0, has_side_effects=True),
        name="exchange",
    )(
        step_index, conditioning, target_state, noise_sample, send_rows,
        sender_weight, edge_weight, receiver_weight, message_weight, output_weight, node_weight,
    )
    w_all = w_all.reshape(devices * rows, 5 * width)
    w_node = w_node.reshape(devices * node_rows, width)
    slots_n = edge_slot.shape[0]
    mesh_count = mesh_features.shape[1]
    block = min(512, slots_n)
    deep = mesh_count + picks + width
    return pl.pallas_call(
        functools.partial(edge_kernel, conditioning.shape[0]),
        out_shape=jax.ShapeDtypeStruct((mesh_count, width), bf16),
        in_specs=[SMEM] + [VMEM] * 13,
        out_specs=VMEM,
        scratch_shapes=[
            pltpu.VMEM((chans, width), f32),
            pltpu.VMEM((8, width), f32),
            pltpu.VMEM((width, deep), bf16),
            pltpu.VMEM((deep, block), bf16),
            pltpu.VMEM((width, width), bf16),
            pltpu.VMEM((width, 2 * width), bf16),
            pltpu.VMEM((width, width), bf16),
            pltpu.VMEM((geom_weight.shape[0], width, 128), f32),
            pltpu.VMEM((4, width, 128), f32),
            pltpu.VMEM((2 * width, mesh_count), bf16),
            pltpu.VMEM((width, mesh_count), f32),
        ],
        compiler_params=params(),
        name="edges",
    )(
        edge_count, fourier, arrived, w_all, w_node, embed_weight, mesh_features, mesh_weight,
        edge_geometry, geom_weight, edge_slot.reshape(1, slots_n), edge_receiver.reshape(1, slots_n),
        noise_weight, film_weight,
    )


def solution(mesh):
    both = P(None, ("member", "node"))
    placed = (
        both, both, both, P("member"), P(None, "node"), P(None, "node"), P("node"), P("node"),
        P("node", None), P("node"), P(), P(), P(), P("node", None), P("node", None), P("node", None),
        P("node", None), P("node", None), P("node", None), P(), P(),
    )
    return jax.shard_map(
        functools.partial(per_device, mesh.shape["node"]),
        mesh=mesh, in_specs=placed, out_specs=P("node", "member"), check_vma=False,
    )
```

```python
import functools

import jax
import jax.numpy as jnp
from jax import lax
from jax.experimental import pallas as pl
from jax.experimental.pallas import tpu as pltpu
from jax.sharding import PartitionSpec as P

STEPS = 20
sigma_top = 80.0
sigma_low = 0.03
rho_power = 7.0
norm_eps = 1e-05
MESH = pl.DeviceIdType.MESH
VMEM = pl.BlockSpec(memory_space=pltpu.VMEM)
SMEM = pl.BlockSpec(memory_space=pltpu.SMEM)
ANY = pl.BlockSpec(memory_space=pl.ANY)
LIMIT = 60 * 1024 * 1024
f32, bf16 = jnp.float32, jnp.bfloat16


def silu(x):
    half = 0.5 * x
    return half + half * jnp.tanh(half)


def turned(x):
    return x.astype(f32).T


def encoder_kernel(
    devices, step_index, count, cond, target, noise, table, embed, mesh_features, mesh_weight, geometry,
    geom_weight, slots, receivers, noise_weight, film_weight, wa, wb, wc, wd, wo, wn, out,
    raw, x, o, w_all, w_node, emb, small, embedded, pick_s, pick_r, partial, sender_t, recv_t,
    edge_t, msg_t, node_t, out_t, geom_b, film_b, joined, total,
    local, ready_r, ready_l, pair, send, recv, long_s, long_r, near_s, near_r, side_s, side_r,
    part_s, part_r,
):
    chips = devices // 2
    half = chips // 2
    me = lax.axis_index("node")
    z, c = me // 2, lax.rem(me, 2)
    group = lax.axis_index("member")
    lane = lax.rem(group, 4)
    first = group - lane
    sides = [first + lax.rem(lane + k, 2) + 2 * lax.rem(lane // 2 + k // 2, 2) for k in (1, 2)]
    sides.append(first + lax.rem(lane + 1, 2) + 2 * lax.rem(lane // 2 + 1, 2))

    def chip(k):
        return lax.rem(z + k + 2 * chips, chips)

    def at(k):
        return {"node": chip(k) * 2 + c}

    part = {"node": z * 2 + 1 - c}
    right, left, far_r, far_l = at(1), at(-1), at(4), at(-4)
    barrier = pltpu.get_barrier_semaphore()
    greeted = [right, left, far_r, far_l, part] + [{"member": s} for s in sides]
    for t in greeted:
        pl.semaphore_signal(barrier, inc=1, device_id=t, device_id_type=MESH)
    rows, width = wa.shape
    node_rows = wn.shape[0]
    picks = x.shape[0]
    cap = picks // devices
    wide = w_all.shape[3] // 4
    node_wide = w_node.shape[3] // 4
    own = [
        pltpu.make_async_copy(w, w_all.at[z, c, :, width * k : width * (k + 1)], local.at[k])
        for k, w in enumerate((wa, wb, wc, wd, wo))
    ]
    own.append(pltpu.make_async_copy(wn, w_node.at[z, c], local.at[5]))
    for copy in own:
        copy.start()
    for copy in own:
        copy.wait()
    refs = (
        lambda n: w_all.at[n, c, :, pl.ds(pl.multiple_of(lane * wide, 128), wide)],
        lambda n: w_node.at[n, c, :, pl.ds(pl.multiple_of(lane * node_wide, 128), node_wide)],
    )

    def piece(n, target, s, r):
        return [
            pltpu.make_async_remote_copy(
                src_ref=ref(n), dst_ref=ref(n), send_sem=s(k), recv_sem=r(k),
                device_id=target, device_id_type=MESH,
            )
            for k, ref in enumerate(refs)
        ]

    def start(copies):
        for copy in copies:
            copy.start()

    def landed(copies):
        for copy in copies:
            copy.wait_recv()

    def long_hop(e, n, target):
        return piece(n, target, lambda k: long_s.at[k, e], lambda k: long_r.at[k, e])

    def near(kind, e, n):
        target = left if kind == 2 else right
        return piece(n, target, lambda k: near_s.at[kind, k, e], lambda k: near_r.at[kind, k, e])

    def aside(n):
        for p, s in enumerate(sides):
            start(piece(n, {"member": s}, lambda k: side_s.at[p, k], lambda k: side_r.at[p, k]))

    def spread(e, n):
        start(near(0, e, n))
        start(near(2, e, n))

    pl.semaphore_wait(barrier, len(greeted))
    pl.semaphore_signal(pair, inc=1, device_id=part, device_id_type=MESH)
    start(long_hop(1, z, far_r))
    start(long_hop(5, z, far_l))
    spread(0, z)

    def announce(k):
        @pl.when(k < half)
        def _():
            pl.semaphore_signal(ready_r.at[k + 1], inc=1, device_id=left, device_id_type=MESH)

        @pl.when(k < half - 1)
        def _():
            pl.semaphore_signal(ready_l.at[k + 1], inc=1, device_id=right, device_id_type=MESH)

    pl.semaphore_wait(pair, 1)
    announce(1)

    vars_ = target.shape[0]
    chans, points_n = raw.shape
    lead = chans - cond.shape[0]
    frac = jnp.full((1, 128), step_index[0], jnp.int32).astype(f32) / (STEPS - 1)
    upper = sigma_top ** (1.0 / rho_power)
    lower = sigma_low ** (1.0 / rho_power)
    base = upper + frac * (lower - upper)
    square = base * base
    sigma = square * square * square * base
    scale = jnp.sqrt(sigma * sigma + 1.0)
    for j in range(points_n // 128):
        lanes = slice(128 * j, 128 * (j + 1))
        raw[0:vars_, lanes] = (target[:, lanes] + sigma * noise[:, lanes]) / scale
    if lead > vars_:
        raw[vars_:lead] = jnp.zeros((lead - vars_, points_n), f32)
    raw[lead:chans] = cond[...].astype(f32)
    spot = lax.broadcasted_iota(jnp.int32, (devices, picks), 1)
    expand = jnp.where(spot // cap == lax.broadcasted_iota(jnp.int32, (devices, picks), 0), 1.0, 0.0).astype(bf16)
    entries = table[...]
    high, low = [
        jnp.dot(half_.astype(f32).astype(bf16), expand, preferred_element_type=f32)
        for half_ in (entries // 32, lax.rem(entries, 32))
    ]
    spot = lax.broadcasted_iota(jnp.int32, (cap, picks), 1)
    mine = lax.rem(spot, cap) == lax.broadcasted_iota(jnp.int32, (cap, picks), 0)
    wanted = jnp.sum(jnp.where(mine, high * 32.0 + low, 0.0), axis=0, keepdims=True).astype(jnp.int32)
    values = raw[...].astype(bf16)
    ids = lax.broadcasted_iota(jnp.int32, (points_n, picks), 0)
    one_hot = jnp.where(ids == wanted, 1.0, 0.0).astype(bf16)
    x[...] = jnp.dot(values, one_hot, preferred_element_type=f32).T.astype(bf16)

    def block(ref, n):
        return ref.at[pl.ds(pl.multiple_of(n * cap, cap), cap)]

    o[pl.ds(pl.multiple_of(me * cap, cap), cap)] = x[pl.ds(pl.multiple_of(me * cap, cap), cap)]

    def points(i, n):
        return pltpu.make_async_remote_copy(
            src_ref=block(x, n), dst_ref=block(o, me), send_sem=send.at[i], recv_sem=recv.at[i],
            device_id={"node": n}, device_id_type=MESH,
        )

    def offer(k):
        for other in (0, 1):
            points(k * 4 + other, chip(k) * 2 + lax.rem(c + other, 2)).start()

            @pl.when(k < half)
            def _():
                points(k * 4 + 2 + other, chip(-k) * 2 + lax.rem(c + other, 2)).start()

    def hear(k):
        pl.semaphore_wait(ready_r.at[k], 1)

        @pl.when(k < half)
        def _():
            pl.semaphore_wait(ready_l.at[k], 1)

    points(0, z * 2 + 1 - c).start()
    offer(1)
    reach = chips // 8

    def rounds(j, carry):
        @pl.when(j <= reach)
        def _():
            n = chip(-4 * j)
            landed(long_hop(j, n, far_r))

            @pl.when(j < reach)
            def _():
                start(long_hop(j + 1, n, far_r))

            spread(j, n)
            aside(n)

        @pl.when(j < reach)
        def _():
            n = chip(4 * j)
            landed(long_hop(4 + j, n, far_l))

            @pl.when(j < reach - 1)
            def _():
                start(long_hop(5 + j, n, far_l))

            spread(4 + j, n)
            aside(n)

        def from_near(e, shift):
            n = chip(shift - 1)
            landed(near(0, e, n))
            start(near(1, e, n))
            aside(n)
            m = chip(shift + 1)
            landed(near(2, e, m))
            aside(m)

        def from_two(e, shift):
            n = chip(shift - 2)
            landed(near(1, e, n))
            aside(n)

        for t in range(4):
            k = 4 * j - 2 + t

            @pl.when(k <= half)
            def _():
                hear(k)
                announce(k)
                offer(k)

        i = j - 1

        @pl.when(i <= reach)
        def _():
            from_near(i, -4 * i)

        @pl.when((i >= 1) & (i < reach))
        def _():
            from_near(4 + i, 4 * i)

        h = j - 2

        @pl.when(h >= 0)
        def _():
            from_two(h, -4 * h)

        @pl.when((h >= 1) & (h < reach))
        def _():
            from_two(4 + h, 4 * h)

        return carry

    lax.fori_loop(1, reach + 3, rounds, 0)

    width = embed.shape[1]
    mesh_count = mesh_features.shape[1]
    batch = min(512, slots.shape[1])
    blocks = slots.shape[1] // batch
    k_mesh, k_geom = mesh_weight.shape[0], geom_weight.shape[0]
    small[0:k_mesh] = mesh_weight[...]
    small[k_mesh : k_mesh + k_geom] = geom_weight[...]
    small[k_mesh + k_geom : 8] = jnp.zeros((8 - k_mesh - k_geom, width), f32)
    small_t = small[...].T
    for k in range(k_geom):
        geom_b[k] = jnp.broadcast_to(small_t[:, k_mesh + k : k_mesh + k + 1], (width, 128))

    def prepare(b, carry):
        first_ = pl.multiple_of(b * batch, batch)
        lanes = lax.broadcasted_iota(jnp.int32, (1, batch), 1) + first_
        here = jnp.where(lanes < count[0], receivers[:, pl.ds(first_, batch)], -1)
        ids = lax.broadcasted_iota(jnp.int32, (mesh_count, batch), 0)
        pick_r[:, pl.ds(first_, batch)] = jnp.where(ids == here, 1.0, 0.0).astype(bf16)
        ids = lax.broadcasted_iota(jnp.int32, (picks, batch), 0)
        pick_s[:, pl.ds(first_, batch)] = jnp.where(ids == slots[:, pl.ds(first_, batch)], 1.0, 0.0).astype(bf16)
        for j in range(batch // 128):
            spot_ = pl.ds(pl.multiple_of(first_ + 128 * j, 128), 128)
            geo = geometry[:, spot_]
            pre = geom_b[0] * geo[0:1]
            for k in range(1, k_geom):
                pre = pre + geom_b[k] * geo[k : k + 1]
            embedded[:, spot_] = silu(pre).astype(bf16)
        return carry

    lax.fori_loop(0, blocks, prepare, 0)

    def quarter(q):
        return (
            w_all.at[0 : chips - 1, c, :, wide * q : wide * (q + 1)],
            w_node.at[0 : chips - 1, c, :, node_wide * q : node_wide * (q + 1)],
        )

    def side_all(p):
        return [
            pltpu.make_async_remote_copy(
                src_ref=ref, dst_ref=ref, send_sem=side_s.at[p, k], recv_sem=side_r.at[p, k],
                device_id={"member": sides[p]}, device_id_type=MESH,
            )
            for k, ref in enumerate(quarter(0))
        ]

    for p in range(3):
        landed(side_all(p))
    over = [
        pltpu.make_async_remote_copy(
            src_ref=ref.at[:, c], dst_ref=ref.at[:, c], send_sem=part_s.at[k], recv_sem=part_r.at[k],
            device_id=part, device_id_type=MESH,
        )
        for k, ref in enumerate((w_all, w_node))
    ]
    start(over)
    angle = 0.25 * jnp.log(sigma[:, 0:1]) * (
        lax.broadcasted_iota(jnp.int32, (noise_weight.shape[0] // 2, 1), 0).astype(f32) + 1.0
    )
    freqs = noise_weight.shape[0] // 2
    level = jnp.sum(jnp.sin(angle) * noise_weight[0:freqs], axis=0, keepdims=True)
    level = level + jnp.sum(jnp.cos(angle) * noise_weight[freqs:], axis=0, keepdims=True)
    level = silu(level).astype(bf16).astype(f32)
    level = jnp.broadcast_to(level, (8, width)).astype(bf16)
    for k in range(4):
        film = jnp.dot(level, film_weight[:, width * k : width * (k + 1)], preferred_element_type=f32)
        column = film.T[:, 0:1]
        if k % 2 == 0:
            column = column + 1.0
        film_b[k] = jnp.broadcast_to(column, (width, 128))
    pre = small_t[:, 0:1] * mesh_features[0:1, :]
    for k in range(1, k_mesh):
        pre = pre + small_t[:, k : k + 1] * mesh_features[k : k + 1, :]
    joined[0:width] = silu(pre).astype(bf16)
    cond_rows = cond.shape[0]
    rest = embed.shape[0] - cond_rows
    emb[0:rest] = embed[cond_rows:, :].astype(f32)
    if lead > rest:
        emb[rest:lead] = jnp.zeros((lead - rest, width), f32)
    emb[lead:chans] = embed[0:cond_rows, :].astype(f32)
    emb_t = emb[...].T.astype(bf16)
    total[...] = jnp.zeros_like(total)
    landed(over)

    def weight(k):
        return w_all[:, :, :, width * k : width * (k + 1)].reshape(width, width)

    edge_t[...] = turned(weight(1)).astype(bf16)
    recv_t[...] = jnp.dot(
        turned(weight(2)).astype(bf16), joined[0:width], preferred_element_type=f32
    ).astype(bf16)

    def before_senders(b, carry):
        spot_ = pl.ds(pl.multiple_of(b * batch, batch), batch)
        value = jnp.dot(edge_t[...], embedded[:, spot_], preferred_element_type=f32)
        partial[:, spot_] = value + jnp.dot(recv_t[...], pick_r[:, spot_], preferred_element_type=f32)
        return carry

    lax.fori_loop(0, blocks, before_senders, 0)
    send_t = turned(weight(0)).astype(bf16)
    msg_t[...] = turned(weight(3)).astype(bf16)
    out_t[...] = turned(weight(4)).astype(bf16)
    node_t[...] = turned(w_node[...].reshape(2 * width, width)).astype(bf16)

    def arrive(k, carry):
        for j in range(2):
            points(k * 4 + j, me).wait_recv()

            @pl.when(k < half)
            def _():
                points(k * 4 + 2 + j, me).wait_recv()

        return carry

    points(0, me).wait_recv()
    lax.fori_loop(1, half + 1, arrive, 0)
    latent = silu(
        lax.dot_general(emb_t, o[...], (((1,), (1,)), ((), ())), preferred_element_type=f32)
    ).astype(bf16)
    sender_t[...] = jnp.dot(send_t, latent, preferred_element_type=f32).astype(bf16)

    def norm(values):
        mean = jnp.mean(values, axis=0, keepdims=True)
        centred = values - mean
        var = jnp.mean(centred * centred, axis=0, keepdims=True)
        return centred * lax.rsqrt(var + norm_eps)

    def add_block(b, carry):
        spot_ = pl.ds(pl.multiple_of(b * batch, batch), batch)
        pre = partial[:, spot_] + jnp.dot(sender_t[...], pick_s[:, spot_], preferred_element_type=f32)
        hidden = silu(pre).astype(bf16)
        normed = norm(jnp.dot(msg_t[...], hidden, preferred_element_type=f32))
        message = jnp.concatenate(
            [
                (normed[:, 128 * j : 128 * (j + 1)] * film_b[0] + film_b[1]).astype(bf16)
                for j in range(batch // 128)
            ],
            axis=1,
        )
        total[...] += lax.dot_general(
            message, pick_r[:, spot_], (((1,), (1,)), ((), ())), preferred_element_type=f32
        )
        return carry

    lax.fori_loop(0, blocks, add_block, 0)
    for p in range(3):
        for copy in side_all(p):
            copy.wait_send()

    def sent(e, carry):
        @pl.when(e > 0)
        def _():
            for copy in long_hop(e, z, far_r):
                copy.wait_send()

        for kind in range(3):
            for copy in near(kind, e, z):
                copy.wait_send()

        return carry

    lax.fori_loop(0, 2 * reach, sent, 0)

    for copy in over:
        copy.wait_send()


    def left_(k, carry):
        for j in range(2):
            points(k * 4 + j, me).wait_send()

            @pl.when(k < half)
            def _():
                points(k * 4 + 2 + j, me).wait_send()

        return carry

    points(0, me).wait_send()
    lax.fori_loop(1, half + 1, left_, 0)
    joined[width : 2 * width] = total[...].astype(bf16)
    update = silu(jnp.dot(node_t[...], joined[...], preferred_element_type=f32)).astype(bf16)
    normed = norm(jnp.dot(out_t[...], update, preferred_element_type=f32))
    for j in range(mesh_count // 128):
        lanes = slice(128 * j, 128 * (j + 1))
        value = joined[0:width, lanes].astype(f32) + normed[:, lanes] * film_b[2] + film_b[3]
        out[lanes, :] = value.T.astype(bf16)


def per_device(
    devices, conditioning, target_state, noise_sample, step_index, mesh_features, edge_geometry,
    edge_slot, edge_receiver, send_rows, edge_count, embed_weight, mesh_weight, geom_weight,
    sender_weight, edge_weight, receiver_weight, message_weight, node_weight, output_weight,
    noise_weight, film_weight,
):
    width = embed_weight.shape[1]
    points = conditioning.shape[1]
    chans = (conditioning.shape[0] + target_state.shape[0] + 7) // 8 * 8
    picks = send_rows.size
    slots_n = edge_slot.shape[0]
    mesh_count = mesh_features.shape[1]
    chips = devices // 2
    half = chips // 2
    sem = pltpu.SemaphoreType
    rows, node_rows = sender_weight.shape[0], node_weight.shape[0]
    return pl.pallas_call(
        functools.partial(encoder_kernel, devices),
        out_shape=jax.ShapeDtypeStruct((mesh_count, width), bf16),
        in_specs=[SMEM] * 2 + [VMEM] * 13 + [ANY] * 6,
        out_specs=VMEM,
        scratch_shapes=[
            pltpu.VMEM((chans, points), f32),
            pltpu.VMEM((picks, chans), bf16),
            pltpu.VMEM((picks, chans), bf16),
            pltpu.VMEM((chips, 2, rows, 5 * width), bf16),
            pltpu.VMEM((chips, 2, node_rows, width), bf16),
            pltpu.VMEM((chans, width), f32),
            pltpu.VMEM((8, width), f32),
            pltpu.VMEM((width, slots_n), bf16),
            pltpu.VMEM((picks, slots_n), bf16),
            pltpu.VMEM((mesh_count, slots_n), bf16),
            pltpu.VMEM((width, slots_n), f32),
            pltpu.VMEM((width, picks), bf16),
            pltpu.VMEM((width, mesh_count), bf16),
            pltpu.VMEM((width, width), bf16),
            pltpu.VMEM((width, width), bf16),
            pltpu.VMEM((width, 2 * width), bf16),
            pltpu.VMEM((width, width), bf16),
            pltpu.VMEM((geom_weight.shape[0], width, 128), f32),
            pltpu.VMEM((4, width, 128), f32),
            pltpu.VMEM((2 * width, mesh_count), bf16),
            pltpu.VMEM((width, mesh_count), f32),
            sem.DMA((6,)),
            sem.REGULAR((half + 1,)),
            sem.REGULAR((half + 1,)),
            sem.REGULAR,
            sem.DMA((4 * half + 4,)),
            sem.DMA((4 * half + 4,)),
            sem.DMA((2, chips // 4)),
            sem.DMA((2, chips // 4)),
            sem.DMA((3, 2, chips // 4)),
            sem.DMA((3, 2, chips // 4)),
            sem.DMA((3, 2)),
            sem.DMA((3, 2)),
            sem.DMA((2,)),
            sem.DMA((2,)),
        ],
        compiler_params=pltpu.CompilerParams(
            vmem_limit_bytes=LIMIT, collective_id=0, has_side_effects=True
        ),
        name="encoder",
    )(
        step_index, edge_count, conditioning, target_state, noise_sample, send_rows.T, embed_weight,
        mesh_features, mesh_weight, edge_geometry, geom_weight, edge_slot.reshape(1, slots_n),
        edge_receiver.reshape(1, slots_n), noise_weight, film_weight, sender_weight, edge_weight,
        receiver_weight, message_weight, output_weight, node_weight,
    )


def solution(mesh):
    both = P(None, ("member", "node"))
    placed = (
        both, both, both, P("member"), P(None, "node"), P(None, "node"), P("node"), P("node"),
        P("node", None), P("node"), P(), P(), P(), P("node", None), P("node", None), P("node", None),
        P("node", None), P("node", None), P("node", None), P(), P(),
    )
    return jax.shard_map(
        functools.partial(per_device, mesh.shape["node"]),
        mesh=mesh, in_specs=placed, out_specs=P("node", "member"), check_vma=False,
    )
```

```python
import functools

import jax
import jax.numpy as jnp
from jax import lax
from jax.experimental import pallas as pl
from jax.experimental.pallas import tpu as pltpu
from jax.sharding import PartitionSpec as P

STEPS = 20
sigma_top = 80.0
sigma_low = 0.03
rho_power = 7.0
norm_eps = 1e-05
MESH = pl.DeviceIdType.MESH
VMEM = pl.BlockSpec(memory_space=pltpu.VMEM)
SMEM = pl.BlockSpec(memory_space=pltpu.SMEM)
ANY = pl.BlockSpec(memory_space=pl.ANY)
LIMIT = 60 * 1024 * 1024
f32, bf16 = jnp.float32, jnp.bfloat16


def silu(x):
    half = 0.5 * x
    return half + half * jnp.tanh(half)


def turned(x):
    return x.astype(f32).T


def encoder_kernel(
    devices, step_index, count, table, mesh_features, mesh_weight, geom_weight, slots, receivers,
    noise_weight, cond_in, target_in, noise_in, geometry_in, embed_in, film_in, wa, wb, wc, wd, wo, wn, out,
    cond, target, noise, geometry, embed, film_weight, raw, x, o, w_all, w_node, emb, small, embedded, pick_s, pick_r, partial, sender_t, recv_t,
    edge_t, msg_t, node_t, out_t, geom_b, film_b, joined, total,
    local, fetch, ready_r, ready_l, pair, pair_done, send, recv, long_s, long_r, near_s, near_r, side_s, side_r,
    part_s, part_r,
):
    chips = devices // 2
    half = chips // 2
    me = lax.axis_index("node")
    z, c = me // 2, lax.rem(me, 2)
    group = lax.axis_index("member")
    lane = lax.rem(group, 4)
    first = group - lane
    sides = [first + lax.rem(lane + k, 2) + 2 * lax.rem(lane // 2 + k // 2, 2) for k in (1, 2)]
    sides.append(first + lax.rem(lane + 1, 2) + 2 * lax.rem(lane // 2 + 1, 2))

    def chip(k):
        return lax.rem(z + k + 2 * chips, chips)

    def at(k):
        return {"node": chip(k) * 2 + c}

    part = {"node": z * 2 + 1 - c}
    right, left, far_r, far_l = at(1), at(-1), at(4), at(-4)
    barrier = pltpu.get_barrier_semaphore()
    greeted = [right, left, far_r, far_l, part] + [{"member": s} for s in sides]
    for t in greeted:
        pl.semaphore_signal(barrier, inc=1, device_id=t, device_id_type=MESH)
    fetched = [
        pltpu.make_async_copy(src, dst, fetch.at[k])
        for k, (src, dst) in enumerate(
            (
                (target_in, target), (noise_in, noise), (cond_in, cond),
                (geometry_in, geometry), (embed_in, embed), (film_in, film_weight),
            )
        )
    ]
    rows, width = wa.shape
    node_rows = wn.shape[0]
    picks = x.shape[0]
    cap = picks // devices
    wide = w_all.shape[3] // 4
    node_wide = w_node.shape[3] // 4
    own = [
        pltpu.make_async_copy(w, w_all.at[z, c, :, width * k : width * (k + 1)], local.at[k])
        for k, w in enumerate((wa, wb, wc, wd, wo))
    ]
    own.append(pltpu.make_async_copy(wn, w_node.at[z, c], local.at[5]))
    for copy in own + fetched:
        copy.start()
    for copy in own:
        copy.wait()
    refs = (
        lambda n: w_all.at[n, c, :, pl.ds(pl.multiple_of(lane * wide, 128), wide)],
        lambda n: w_node.at[n, c, :, pl.ds(pl.multiple_of(lane * node_wide, 128), node_wide)],
    )

    def piece(n, target, s, r):
        return [
            pltpu.make_async_remote_copy(
                src_ref=ref(n), dst_ref=ref(n), send_sem=s(k), recv_sem=r(k),
                device_id=target, device_id_type=MESH,
            )
            for k, ref in enumerate(refs)
        ]

    def start(copies):
        for copy in copies:
            copy.start()

    def landed(copies):
        for copy in copies:
            copy.wait_recv()

    def long_hop(e, n, target):
        return piece(n, target, lambda k: long_s.at[k, e], lambda k: long_r.at[k, e])

    def near(kind, e, n):
        target = left if kind == 2 else right
        return piece(n, target, lambda k: near_s.at[kind, k, e], lambda k: near_r.at[kind, k, e])

    def aside(n):
        for p, s in enumerate(sides):
            start(piece(n, {"member": s}, lambda k: side_s.at[p, k], lambda k: side_r.at[p, k]))

    def spread(e, n):
        start(near(0, e, n))
        start(near(2, e, n))

    pl.semaphore_wait(barrier, len(greeted))
    pl.semaphore_signal(pair, inc=1, device_id=part, device_id_type=MESH)
    start(long_hop(1, z, far_r))
    start(long_hop(5, z, far_l))
    spread(0, z)

    def announce(k):
        @pl.when(k < half)
        def _():
            pl.semaphore_signal(ready_r.at[k + 1], inc=1, device_id=left, device_id_type=MESH)

        @pl.when(k < half - 1)
        def _():
            pl.semaphore_signal(ready_l.at[k + 1], inc=1, device_id=right, device_id_type=MESH)

    pl.semaphore_wait(pair, 1)
    announce(1)

    for copy in fetched[:3]:
        copy.wait()
    vars_ = target.shape[0]
    chans, points_n = raw.shape
    lead = chans - cond.shape[0]
    frac = jnp.full((1, 128), step_index[0], jnp.int32).astype(f32) / (STEPS - 1)
    upper = sigma_top ** (1.0 / rho_power)
    lower = sigma_low ** (1.0 / rho_power)
    base = upper + frac * (lower - upper)
    square = base * base
    sigma = square * square * square * base
    scale = jnp.sqrt(sigma * sigma + 1.0)
    for j in range(points_n // 128):
        lanes = slice(128 * j, 128 * (j + 1))
        raw[0:vars_, lanes] = (target[:, lanes] + sigma * noise[:, lanes]) / scale
    if lead > vars_:
        raw[vars_:lead] = jnp.zeros((lead - vars_, points_n), f32)
    raw[lead:chans] = cond[...].astype(f32)
    spot = lax.broadcasted_iota(jnp.int32, (devices, picks), 1)
    expand = jnp.where(spot // cap == lax.broadcasted_iota(jnp.int32, (devices, picks), 0), 1.0, 0.0).astype(bf16)
    entries = table[...]
    high, low = [
        jnp.dot(half_.astype(f32).astype(bf16), expand, preferred_element_type=f32)
        for half_ in (entries // 32, lax.rem(entries, 32))
    ]
    spot = lax.broadcasted_iota(jnp.int32, (cap, picks), 1)
    mine = lax.rem(spot, cap) == lax.broadcasted_iota(jnp.int32, (cap, picks), 0)
    wanted = jnp.sum(jnp.where(mine, high * 32.0 + low, 0.0), axis=0, keepdims=True).astype(jnp.int32)
    values = raw[...].astype(bf16)
    ids = lax.broadcasted_iota(jnp.int32, (points_n, picks), 0)
    one_hot = jnp.where(ids == wanted, 1.0, 0.0).astype(bf16)
    x[...] = jnp.dot(values, one_hot, preferred_element_type=f32).T.astype(bf16)

    def block(ref, n):
        return ref.at[pl.ds(pl.multiple_of(n * cap, cap), cap)]

    o[pl.ds(pl.multiple_of(me * cap, cap), cap)] = x[pl.ds(pl.multiple_of(me * cap, cap), cap)]

    def points(i, n):
        return pltpu.make_async_remote_copy(
            src_ref=block(x, n), dst_ref=block(o, me), send_sem=send.at[i], recv_sem=recv.at[i],
            device_id={"node": n}, device_id_type=MESH,
        )

    def offer(k):
        for other in (0, 1):
            points(k * 4 + other, chip(k) * 2 + lax.rem(c + other, 2)).start()

            @pl.when(k < half)
            def _():
                points(k * 4 + 2 + other, chip(-k) * 2 + lax.rem(c + other, 2)).start()

    def hear(k):
        pl.semaphore_wait(ready_r.at[k], 1)

        @pl.when(k < half)
        def _():
            pl.semaphore_wait(ready_l.at[k], 1)

    points(0, z * 2 + 1 - c).start()
    offer(1)
    reach = chips // 8

    def rounds(j, carry):
        @pl.when(j <= reach)
        def _():
            n = chip(-4 * j)
            landed(long_hop(j, n, far_r))

            @pl.when(j < reach)
            def _():
                start(long_hop(j + 1, n, far_r))

            spread(j, n)
            aside(n)

        @pl.when(j < reach)
        def _():
            n = chip(4 * j)
            landed(long_hop(4 + j, n, far_l))

            @pl.when(j < reach - 1)
            def _():
                start(long_hop(5 + j, n, far_l))

            spread(4 + j, n)
            aside(n)

        def from_near(e, shift):
            n = chip(shift - 1)
            landed(near(0, e, n))
            start(near(1, e, n))
            aside(n)
            m = chip(shift + 1)
            landed(near(2, e, m))
            aside(m)

        def from_two(e, shift):
            n = chip(shift - 2)
            landed(near(1, e, n))
            aside(n)

        for t in range(4):
            k = 4 * j - 2 + t

            @pl.when(k <= half)
            def _():
                hear(k)
                announce(k)

        i = j - 1

        @pl.when(i <= reach)
        def _():
            from_near(i, -4 * i)

        @pl.when((i >= 1) & (i < reach))
        def _():
            from_near(4 + i, 4 * i)

        h = j - 2

        @pl.when(h >= 0)
        def _():
            from_two(h, -4 * h)

        @pl.when((h >= 1) & (h < reach))
        def _():
            from_two(4 + h, 4 * h)

        @pl.when(j <= reach)
        def _():
            offer(2 * j)
            offer(2 * j + 1)

        return carry

    lax.fori_loop(1, reach + 3, rounds, 0)

    pl.semaphore_signal(pair_done, inc=1, device_id=part, device_id_type=MESH)
    pl.semaphore_wait(pair_done, 1)

    def rest(t, carry):
        offer(half - t)
        return carry

    lax.fori_loop(0, half - 2 * reach - 1, rest, 0)

    width = embed.shape[1]
    mesh_count = mesh_features.shape[1]
    batch = min(512, slots.shape[1])
    blocks = slots.shape[1] // batch
    k_mesh, k_geom = mesh_weight.shape[0], geom_weight.shape[0]
    for copy in fetched[3:]:
        copy.wait()
    small[0:k_mesh] = mesh_weight[...]
    small[k_mesh : k_mesh + k_geom] = geom_weight[...]
    small[k_mesh + k_geom : 8] = jnp.zeros((8 - k_mesh - k_geom, width), f32)
    small_t = small[...].T
    for k in range(k_geom):
        geom_b[k] = jnp.broadcast_to(small_t[:, k_mesh + k : k_mesh + k + 1], (width, 128))

    def prepare(b, carry):
        first_ = pl.multiple_of(b * batch, batch)
        lanes = lax.broadcasted_iota(jnp.int32, (1, batch), 1) + first_
        here = jnp.where(lanes < count[0], receivers[:, pl.ds(first_, batch)], -1)
        ids = lax.broadcasted_iota(jnp.int32, (mesh_count, batch), 0)
        pick_r[:, pl.ds(first_, batch)] = jnp.where(ids == here, 1.0, 0.0).astype(bf16)
        ids = lax.broadcasted_iota(jnp.int32, (picks, batch), 0)
        pick_s[:, pl.ds(first_, batch)] = jnp.where(ids == slots[:, pl.ds(first_, batch)], 1.0, 0.0).astype(bf16)
        for j in range(batch // 128):
            spot_ = pl.ds(pl.multiple_of(first_ + 128 * j, 128), 128)
            geo = geometry[:, spot_]
            pre = geom_b[0] * geo[0:1]
            for k in range(1, k_geom):
                pre = pre + geom_b[k] * geo[k : k + 1]
            embedded[:, spot_] = silu(pre).astype(bf16)
        return carry

    lax.fori_loop(0, blocks // 2, prepare, 0)

    def quarter(q):
        return (
            w_all.at[0 : chips - 1, c, :, wide * q : wide * (q + 1)],
            w_node.at[0 : chips - 1, c, :, node_wide * q : node_wide * (q + 1)],
        )

    def side_all(p):
        return [
            pltpu.make_async_remote_copy(
                src_ref=ref, dst_ref=ref, send_sem=side_s.at[p, k], recv_sem=side_r.at[p, k],
                device_id={"member": sides[p]}, device_id_type=MESH,
            )
            for k, ref in enumerate(quarter(0))
        ]

    for p in range(3):
        landed(side_all(p))
    over = [
        pltpu.make_async_remote_copy(
            src_ref=ref.at[:, c], dst_ref=ref.at[:, c], send_sem=part_s.at[k], recv_sem=part_r.at[k],
            device_id=part, device_id_type=MESH,
        )
        for k, ref in enumerate((w_all, w_node))
    ]
    start(over)
    lax.fori_loop(blocks // 2, blocks, prepare, 0)
    angle = 0.25 * jnp.log(sigma[:, 0:1]) * (
        lax.broadcasted_iota(jnp.int32, (noise_weight.shape[0] // 2, 1), 0).astype(f32) + 1.0
    )
    freqs = noise_weight.shape[0] // 2
    level = jnp.sum(jnp.sin(angle) * noise_weight[0:freqs], axis=0, keepdims=True)
    level = level + jnp.sum(jnp.cos(angle) * noise_weight[freqs:], axis=0, keepdims=True)
    level = silu(level).astype(bf16).astype(f32)
    level = jnp.broadcast_to(level, (8, width)).astype(bf16)
    for k in range(4):
        film = jnp.dot(level, film_weight[:, width * k : width * (k + 1)], preferred_element_type=f32)
        column = film.T[:, 0:1]
        if k % 2 == 0:
            column = column + 1.0
        film_b[k] = jnp.broadcast_to(column, (width, 128))
    pre = small_t[:, 0:1] * mesh_features[0:1, :]
    for k in range(1, k_mesh):
        pre = pre + small_t[:, k : k + 1] * mesh_features[k : k + 1, :]
    joined[0:width] = silu(pre).astype(bf16)
    cond_rows = cond.shape[0]
    rest = embed.shape[0] - cond_rows
    emb[0:rest] = embed[cond_rows:, :].astype(f32)
    if lead > rest:
        emb[rest:lead] = jnp.zeros((lead - rest, width), f32)
    emb[lead:chans] = embed[0:cond_rows, :].astype(f32)
    emb_t = emb[...].T.astype(bf16)
    total[...] = jnp.zeros_like(total)
    landed(over)

    def weight(k):
        return w_all[:, :, :, width * k : width * (k + 1)].reshape(width, width)

    edge_t[...] = turned(weight(1)).astype(bf16)
    recv_t[...] = jnp.dot(
        turned(weight(2)).astype(bf16), joined[0:width], preferred_element_type=f32
    ).astype(bf16)

    def before_senders(b, carry):
        spot_ = pl.ds(pl.multiple_of(b * batch, batch), batch)
        value = jnp.dot(edge_t[...], embedded[:, spot_], preferred_element_type=f32)
        partial[:, spot_] = value + jnp.dot(recv_t[...], pick_r[:, spot_], preferred_element_type=f32)
        return carry

    lax.fori_loop(0, blocks, before_senders, 0)
    send_t = turned(weight(0)).astype(bf16)
    msg_t[...] = turned(weight(3)).astype(bf16)
    out_t[...] = turned(weight(4)).astype(bf16)
    node_t[...] = turned(w_node[...].reshape(2 * width, width)).astype(bf16)

    def arrive(k, carry):
        for j in range(2):
            points(k * 4 + j, me).wait_recv()

            @pl.when(k < half)
            def _():
                points(k * 4 + 2 + j, me).wait_recv()

        return carry

    points(0, me).wait_recv()
    lax.fori_loop(1, half + 1, arrive, 0)
    latent = silu(
        lax.dot_general(emb_t, o[...], (((1,), (1,)), ((), ())), preferred_element_type=f32)
    ).astype(bf16)
    sender_t[...] = jnp.dot(send_t, latent, preferred_element_type=f32).astype(bf16)

    def norm(values):
        mean = jnp.mean(values, axis=0, keepdims=True)
        centred = values - mean
        var = jnp.mean(centred * centred, axis=0, keepdims=True)
        return centred * lax.rsqrt(var + norm_eps)

    def add_block(b, carry):
        spot_ = pl.ds(pl.multiple_of(b * batch, batch), batch)
        pre = partial[:, spot_] + jnp.dot(sender_t[...], pick_s[:, spot_], preferred_element_type=f32)
        hidden = silu(pre).astype(bf16)
        normed = norm(jnp.dot(msg_t[...], hidden, preferred_element_type=f32))
        message = jnp.concatenate(
            [
                (normed[:, 128 * j : 128 * (j + 1)] * film_b[0] + film_b[1]).astype(bf16)
                for j in range(batch // 128)
            ],
            axis=1,
        )
        total[...] += lax.dot_general(
            message, pick_r[:, spot_], (((1,), (1,)), ((), ())), preferred_element_type=f32
        )
        return carry

    lax.fori_loop(0, blocks, add_block, 0)
    for p in range(3):
        for copy in side_all(p):
            copy.wait_send()

    def sent(e, carry):
        @pl.when(e > 0)
        def _():
            for copy in long_hop(e, z, far_r):
                copy.wait_send()

        for kind in range(3):
            for copy in near(kind, e, z):
                copy.wait_send()

        return carry

    lax.fori_loop(0, 2 * reach, sent, 0)

    for copy in over:
        copy.wait_send()


    def left_(k, carry):
        for j in range(2):
            points(k * 4 + j, me).wait_send()

            @pl.when(k < half)
            def _():
                points(k * 4 + 2 + j, me).wait_send()

        return carry

    points(0, me).wait_send()
    lax.fori_loop(1, half + 1, left_, 0)
    joined[width : 2 * width] = total[...].astype(bf16)
    update = silu(jnp.dot(node_t[...], joined[...], preferred_element_type=f32)).astype(bf16)
    normed = norm(jnp.dot(out_t[...], update, preferred_element_type=f32))
    for j in range(mesh_count // 128):
        lanes = slice(128 * j, 128 * (j + 1))
        value = joined[0:width, lanes].astype(f32) + normed[:, lanes] * film_b[2] + film_b[3]
        out[lanes, :] = value.T.astype(bf16)


def per_device(
    devices, conditioning, target_state, noise_sample, step_index, mesh_features, edge_geometry,
    edge_slot, edge_receiver, send_rows, edge_count, embed_weight, mesh_weight, geom_weight,
    sender_weight, edge_weight, receiver_weight, message_weight, node_weight, output_weight,
    noise_weight, film_weight,
):
    width = embed_weight.shape[1]
    points = conditioning.shape[1]
    chans = (conditioning.shape[0] + target_state.shape[0] + 7) // 8 * 8
    picks = send_rows.size
    slots_n = edge_slot.shape[0]
    mesh_count = mesh_features.shape[1]
    chips = devices // 2
    half = chips // 2
    sem = pltpu.SemaphoreType
    rows, node_rows = sender_weight.shape[0], node_weight.shape[0]
    return pl.pallas_call(
        functools.partial(encoder_kernel, devices),
        out_shape=jax.ShapeDtypeStruct((mesh_count, width), bf16),
        in_specs=[SMEM] * 2 + [VMEM] * 7 + [ANY] * 12,
        out_specs=VMEM,
        scratch_shapes=[
            pltpu.VMEM(conditioning.shape, bf16),
            pltpu.VMEM(target_state.shape, f32),
            pltpu.VMEM(noise_sample.shape, f32),
            pltpu.VMEM(edge_geometry.shape, f32),
            pltpu.VMEM(embed_weight.shape, bf16),
            pltpu.VMEM(film_weight.shape, bf16),
            pltpu.VMEM((chans, points), f32),
            pltpu.VMEM((picks, chans), bf16),
            pltpu.VMEM((picks, chans), bf16),
            pltpu.VMEM((chips, 2, rows, 5 * width), bf16),
            pltpu.VMEM((chips, 2, node_rows, width), bf16),
            pltpu.VMEM((chans, width), f32),
            pltpu.VMEM((8, width), f32),
            pltpu.VMEM((width, slots_n), bf16),
            pltpu.VMEM((picks, slots_n), bf16),
            pltpu.VMEM((mesh_count, slots_n), bf16),
            pltpu.VMEM((width, slots_n), f32),
            pltpu.VMEM((width, picks), bf16),
            pltpu.VMEM((width, mesh_count), bf16),
            pltpu.VMEM((width, width), bf16),
            pltpu.VMEM((width, width), bf16),
            pltpu.VMEM((width, 2 * width), bf16),
            pltpu.VMEM((width, width), bf16),
            pltpu.VMEM((geom_weight.shape[0], width, 128), f32),
            pltpu.VMEM((4, width, 128), f32),
            pltpu.VMEM((2 * width, mesh_count), bf16),
            pltpu.VMEM((width, mesh_count), f32),
            sem.DMA((6,)),
            sem.DMA((6,)),
            sem.REGULAR((half + 1,)),
            sem.REGULAR((half + 1,)),
            sem.REGULAR,
            sem.REGULAR,
            sem.DMA((4 * half + 4,)),
            sem.DMA((4 * half + 4,)),
            sem.DMA((2, chips // 4)),
            sem.DMA((2, chips // 4)),
            sem.DMA((3, 2, chips // 4)),
            sem.DMA((3, 2, chips // 4)),
            sem.DMA((3, 2)),
            sem.DMA((3, 2)),
            sem.DMA((2,)),
            sem.DMA((2,)),
        ],
        compiler_params=pltpu.CompilerParams(
            vmem_limit_bytes=LIMIT, collective_id=0, has_side_effects=True
        ),
        name="encoder",
    )(
        step_index, edge_count, send_rows.T, mesh_features, mesh_weight, geom_weight,
        edge_slot.reshape(1, slots_n), edge_receiver.reshape(1, slots_n), noise_weight,
        conditioning, target_state, noise_sample, edge_geometry, embed_weight, film_weight,
        sender_weight, edge_weight, receiver_weight, message_weight, output_weight, node_weight,
    )


def solution(mesh):
    both = P(None, ("member", "node"))
    placed = (
        both, both, both, P("member"), P(None, "node"), P(None, "node"), P("node"), P("node"),
        P("node", None), P("node"), P(), P(), P(), P("node", None), P("node", None), P("node", None),
        P("node", None), P("node", None), P("node", None), P(), P(),
    )
    return jax.shard_map(
        functools.partial(per_device, mesh.shape["node"]),
        mesh=mesh, in_specs=placed, out_specs=P("node", "member"), check_vma=False,
    )
```

```python
import functools

import jax
import jax.numpy as jnp
from jax import lax
from jax.experimental import pallas as pl
from jax.experimental.pallas import tpu as pltpu
from jax.sharding import PartitionSpec as P

STEPS = 20
sigma_top = 80.0
sigma_low = 0.03
rho_power = 7.0
norm_eps = 1e-05
MESH = pl.DeviceIdType.MESH
VMEM = pl.BlockSpec(memory_space=pltpu.VMEM)
SMEM = pl.BlockSpec(memory_space=pltpu.SMEM)
ANY = pl.BlockSpec(memory_space=pl.ANY)
LIMIT = 60 * 1024 * 1024
f32, bf16 = jnp.float32, jnp.bfloat16


def silu(x):
    half = 0.5 * x
    return half + half * jnp.tanh(half)


def turned(x):
    return x.astype(f32).T


def encoder_kernel(
    devices, step_index, count, table, mesh_features, mesh_weight, geom_weight, slots, receivers,
    noise_weight, cond_in, target_in, noise_in, geometry_in, embed_in, film_in, wa, wb, wc, wd, wo, wn, out,
    cond, target, noise, geometry, embed, film_weight, raw, x, o, w_all, w_node, emb, small, embedded, pick_s, pick_r, partial, sender_t, recv_t,
    edge_t, msg_t, node_t, out_t, geom_b, film_b, joined, total, emb_t, send_t,
    local, fetch, ready_r, ready_l, pair, pair_done, send, recv, long_s, long_r, near_s, near_r, side_s, side_r,
    part_s, part_r,
):
    chips = devices // 2
    half = chips // 2
    me = lax.axis_index("node")
    z, c = me // 2, lax.rem(me, 2)
    group = lax.axis_index("member")
    lane = lax.rem(group, 4)
    first = group - lane
    sides = [first + lax.rem(lane + k, 2) + 2 * lax.rem(lane // 2 + k // 2, 2) for k in (1, 2)]
    sides.append(first + lax.rem(lane + 1, 2) + 2 * lax.rem(lane // 2 + 1, 2))

    def chip(k):
        return lax.rem(z + k + 2 * chips, chips)

    def at(k):
        return {"node": chip(k) * 2 + c}

    part = {"node": z * 2 + 1 - c}
    right, left, far_r, far_l = at(1), at(-1), at(4), at(-4)
    barrier = pltpu.get_barrier_semaphore()
    greeted = [right, left, far_r, far_l, part] + [{"member": s} for s in sides]
    for t in greeted:
        pl.semaphore_signal(barrier, inc=1, device_id=t, device_id_type=MESH)
    fetched = [
        pltpu.make_async_copy(src, dst, fetch.at[k])
        for k, (src, dst) in enumerate(
            (
                (target_in, target), (noise_in, noise), (cond_in, cond),
                (geometry_in, geometry), (embed_in, embed), (film_in, film_weight),
            )
        )
    ]
    rows, width = wa.shape
    node_rows = wn.shape[0]
    picks = x.shape[0]
    cap = picks // devices
    wide = w_all.shape[3] // 4
    node_wide = w_node.shape[3] // 4
    own = [
        pltpu.make_async_copy(w, w_all.at[z, c, :, width * k : width * (k + 1)], local.at[k])
        for k, w in enumerate((wa, wb, wc, wd, wo))
    ]
    own.append(pltpu.make_async_copy(wn, w_node.at[z, c], local.at[5]))
    for copy in own + fetched:
        copy.start()
    for copy in own:
        copy.wait()
    refs = (
        lambda n: w_all.at[n, c, :, pl.ds(pl.multiple_of(lane * wide, 128), wide)],
        lambda n: w_node.at[n, c, :, pl.ds(pl.multiple_of(lane * node_wide, 128), node_wide)],
    )

    def piece(n, target, s, r):
        return [
            pltpu.make_async_remote_copy(
                src_ref=ref(n), dst_ref=ref(n), send_sem=s(k), recv_sem=r(k),
                device_id=target, device_id_type=MESH,
            )
            for k, ref in enumerate(refs)
        ]

    def start(copies):
        for copy in copies:
            copy.start()

    def landed(copies):
        for copy in copies:
            copy.wait_recv()

    def long_hop(e, n, target):
        return piece(n, target, lambda k: long_s.at[k, e], lambda k: long_r.at[k, e])

    def near(kind, e, n):
        target = left if kind == 2 else right
        return piece(n, target, lambda k: near_s.at[kind, k, e], lambda k: near_r.at[kind, k, e])

    def aside(n):
        for p, s in enumerate(sides):
            start(piece(n, {"member": s}, lambda k: side_s.at[p, k], lambda k: side_r.at[p, k]))

    def spread(e, n):
        start(near(0, e, n))
        start(near(2, e, n))

    pl.semaphore_wait(barrier, len(greeted))
    pl.semaphore_signal(pair, inc=1, device_id=part, device_id_type=MESH)
    start(long_hop(1, z, far_r))
    start(long_hop(5, z, far_l))
    spread(0, z)

    def announce(k):
        @pl.when(k < half)
        def _():
            pl.semaphore_signal(ready_r.at[k + 1], inc=1, device_id=left, device_id_type=MESH)

        @pl.when(k < half - 1)
        def _():
            pl.semaphore_signal(ready_l.at[k + 1], inc=1, device_id=right, device_id_type=MESH)

    pl.semaphore_wait(pair, 1)
    announce(1)

    for copy in fetched[:3]:
        copy.wait()
    vars_ = target.shape[0]
    chans, points_n = raw.shape
    lead = chans - cond.shape[0]
    frac = jnp.full((1, 128), step_index[0], jnp.int32).astype(f32) / (STEPS - 1)
    upper = sigma_top ** (1.0 / rho_power)
    lower = sigma_low ** (1.0 / rho_power)
    base = upper + frac * (lower - upper)
    square = base * base
    sigma = square * square * square * base
    scale = jnp.sqrt(sigma * sigma + 1.0)
    for j in range(points_n // 128):
        lanes = slice(128 * j, 128 * (j + 1))
        raw[0:vars_, lanes] = (target[:, lanes] + sigma * noise[:, lanes]) / scale
    if lead > vars_:
        raw[vars_:lead] = jnp.zeros((lead - vars_, points_n), f32)
    raw[lead:chans] = cond[...].astype(f32)
    spot = lax.broadcasted_iota(jnp.int32, (devices, picks), 1)
    expand = jnp.where(spot // cap == lax.broadcasted_iota(jnp.int32, (devices, picks), 0), 1.0, 0.0).astype(bf16)
    entries = table[...]
    high, low = [
        jnp.dot(half_.astype(f32).astype(bf16), expand, preferred_element_type=f32)
        for half_ in (entries // 32, lax.rem(entries, 32))
    ]
    spot = lax.broadcasted_iota(jnp.int32, (cap, picks), 1)
    mine = lax.rem(spot, cap) == lax.broadcasted_iota(jnp.int32, (cap, picks), 0)
    wanted = jnp.sum(jnp.where(mine, high * 32.0 + low, 0.0), axis=0, keepdims=True).astype(jnp.int32)
    values = raw[...].astype(bf16)
    ids = lax.broadcasted_iota(jnp.int32, (points_n, picks), 0)
    one_hot = jnp.where(ids == wanted, 1.0, 0.0).astype(bf16)
    x[...] = jnp.dot(values, one_hot, preferred_element_type=f32).T.astype(bf16)

    def block(ref, n):
        return ref.at[pl.ds(pl.multiple_of(n * cap, cap), cap)]

    around = chips // 4
    o[pl.ds(pl.multiple_of((around * 2 + c) * cap, cap), cap)] = x[pl.ds(pl.multiple_of(me * cap, cap), cap)]

    def points(i, n, seen=0):
        return pltpu.make_async_remote_copy(
            src_ref=block(x, n), dst_ref=block(o, seen * 2 + c), send_sem=send.at[i], recv_sem=recv.at[i],
            device_id={"node": n}, device_id_type=MESH,
        )

    def offer(k):
        for other in (0, 1):
            points(
                k * 4 + other, chip(k) * 2 + lax.rem(c + other, 2), lax.rem(around - k + chips, chips)
            ).start()

            @pl.when(k < half)
            def _():
                points(
                    k * 4 + 2 + other, chip(-k) * 2 + lax.rem(c + other, 2), lax.rem(around + k, chips)
                ).start()

    def hear(k):
        pl.semaphore_wait(ready_r.at[k], 1)

        @pl.when(k < half)
        def _():
            pl.semaphore_wait(ready_l.at[k], 1)

    points(0, z * 2 + 1 - c, around).start()
    offer(1)
    reach = chips // 8

    def rounds(j, carry):
        @pl.when(j <= reach)
        def _():
            n = chip(-4 * j)
            landed(long_hop(j, n, far_r))

            @pl.when(j < reach)
            def _():
                start(long_hop(j + 1, n, far_r))

            spread(j, n)
            aside(n)

        @pl.when(j < reach)
        def _():
            n = chip(4 * j)
            landed(long_hop(4 + j, n, far_l))

            @pl.when(j < reach - 1)
            def _():
                start(long_hop(5 + j, n, far_l))

            spread(4 + j, n)
            aside(n)

        def from_near(e, shift):
            n = chip(shift - 1)
            landed(near(0, e, n))
            start(near(1, e, n))
            aside(n)
            m = chip(shift + 1)
            landed(near(2, e, m))
            aside(m)

        def from_two(e, shift):
            n = chip(shift - 2)
            landed(near(1, e, n))
            aside(n)

        for t in range(4):
            k = 4 * j - 2 + t

            @pl.when(k <= half)
            def _():
                hear(k)
                announce(k)

        i = j - 1

        @pl.when(i <= reach)
        def _():
            from_near(i, -4 * i)

        @pl.when((i >= 1) & (i < reach))
        def _():
            from_near(4 + i, 4 * i)

        h = j - 2

        @pl.when(h >= 0)
        def _():
            from_two(h, -4 * h)

        @pl.when((h >= 1) & (h < reach))
        def _():
            from_two(4 + h, 4 * h)

        @pl.when(j <= reach)
        def _():
            offer(2 * j)
            offer(2 * j + 1)

        return carry

    lax.fori_loop(1, reach + 3, rounds, 0)

    pl.semaphore_signal(pair_done, inc=1, device_id=part, device_id_type=MESH)
    pl.semaphore_wait(pair_done, 1)

    def rest(t, carry):
        offer(half - t)
        return carry

    lax.fori_loop(0, half - 2 * reach - 1, rest, 0)

    width = embed.shape[1]
    mesh_count = mesh_features.shape[1]
    batch = min(512, slots.shape[1])
    blocks = slots.shape[1] // batch
    k_mesh, k_geom = mesh_weight.shape[0], geom_weight.shape[0]
    for copy in fetched[3:]:
        copy.wait()
    small[0:k_mesh] = mesh_weight[...]
    small[k_mesh : k_mesh + k_geom] = geom_weight[...]
    small[k_mesh + k_geom : 8] = jnp.zeros((8 - k_mesh - k_geom, width), f32)
    small_t = small[...].T
    for k in range(k_geom):
        geom_b[k] = jnp.broadcast_to(small_t[:, k_mesh + k : k_mesh + k + 1], (width, 128))

    def prepare(b, carry):
        first_ = pl.multiple_of(b * batch, batch)
        lanes = lax.broadcasted_iota(jnp.int32, (1, batch), 1) + first_
        here = jnp.where(lanes < count[0], receivers[:, pl.ds(first_, batch)], -1)
        ids = lax.broadcasted_iota(jnp.int32, (mesh_count, batch), 0)
        pick_r[:, pl.ds(first_, batch)] = jnp.where(ids == here, 1.0, 0.0).astype(bf16)
        shifted = lax.rem(slots[:, pl.ds(first_, batch)] + (chips + around - z) * 2 * cap, picks)
        ids = lax.broadcasted_iota(jnp.int32, (picks, batch), 0)
        pick_s[:, pl.ds(first_, batch)] = jnp.where(ids == shifted, 1.0, 0.0).astype(bf16)
        for j in range(batch // 128):
            spot_ = pl.ds(pl.multiple_of(first_ + 128 * j, 128), 128)
            geo = geometry[:, spot_]
            pre = geom_b[0] * geo[0:1]
            for k in range(1, k_geom):
                pre = pre + geom_b[k] * geo[k : k + 1]
            embedded[:, spot_] = silu(pre).astype(bf16)
        return carry

    lax.fori_loop(0, blocks // 2, prepare, 0)

    def quarter(q):
        return (
            w_all.at[0 : chips - 1, c, :, wide * q : wide * (q + 1)],
            w_node.at[0 : chips - 1, c, :, node_wide * q : node_wide * (q + 1)],
        )

    def side_all(p):
        return [
            pltpu.make_async_remote_copy(
                src_ref=ref, dst_ref=ref, send_sem=side_s.at[p, k], recv_sem=side_r.at[p, k],
                device_id={"member": sides[p]}, device_id_type=MESH,
            )
            for k, ref in enumerate(quarter(0))
        ]

    for p in range(3):
        landed(side_all(p))
    over = [
        pltpu.make_async_remote_copy(
            src_ref=ref.at[:, c], dst_ref=ref.at[:, c], send_sem=part_s.at[k], recv_sem=part_r.at[k],
            device_id=part, device_id_type=MESH,
        )
        for k, ref in enumerate((w_all, w_node))
    ]
    start(over)
    lax.fori_loop(blocks // 2, blocks, prepare, 0)
    angle = 0.25 * jnp.log(sigma[:, 0:1]) * (
        lax.broadcasted_iota(jnp.int32, (noise_weight.shape[0] // 2, 1), 0).astype(f32) + 1.0
    )
    freqs = noise_weight.shape[0] // 2
    level = jnp.sum(jnp.sin(angle) * noise_weight[0:freqs], axis=0, keepdims=True)
    level = level + jnp.sum(jnp.cos(angle) * noise_weight[freqs:], axis=0, keepdims=True)
    level = silu(level).astype(bf16).astype(f32)
    level = jnp.broadcast_to(level, (8, width)).astype(bf16)
    for k in range(4):
        film = jnp.dot(level, film_weight[:, width * k : width * (k + 1)], preferred_element_type=f32)
        column = film.T[:, 0:1]
        if k % 2 == 0:
            column = column + 1.0
        film_b[k] = jnp.broadcast_to(column, (width, 128))
    pre = small_t[:, 0:1] * mesh_features[0:1, :]
    for k in range(1, k_mesh):
        pre = pre + small_t[:, k : k + 1] * mesh_features[k : k + 1, :]
    joined[0:width] = silu(pre).astype(bf16)
    cond_rows = cond.shape[0]
    rest = embed.shape[0] - cond_rows
    emb[0:rest] = embed[cond_rows:, :].astype(f32)
    if lead > rest:
        emb[rest:lead] = jnp.zeros((lead - rest, width), f32)
    emb[lead:chans] = embed[0:cond_rows, :].astype(f32)
    emb_t[...] = emb[...].T.astype(bf16)
    total[...] = jnp.zeros_like(total)
    landed(over)

    def weight(k):
        return w_all[:, :, :, width * k : width * (k + 1)].reshape(width, width)

    edge_t[...] = turned(weight(1)).astype(bf16)
    recv_t[...] = jnp.dot(
        turned(weight(2)).astype(bf16), joined[0:width], preferred_element_type=f32
    ).astype(bf16)

    near_rows = picks // 2

    def embed_rows(rows_):
        latent = silu(
            lax.dot_general(emb_t[...], o[rows_], (((1,), (1,)), ((), ())), preferred_element_type=f32)
        ).astype(bf16)
        sender_t[:, rows_] = jnp.dot(send_t[...], latent, preferred_element_type=f32).astype(bf16)

    send_t[...] = turned(weight(0)).astype(bf16)

    def arrive_near(k, carry):
        for j in range(2):
            points(k * 4 + j, me).wait_recv()

            @pl.when(k < around)
            def _():
                points(k * 4 + 2 + j, me).wait_recv()

        return carry

    points(0, me).wait_recv()
    lax.fori_loop(1, around + 1, arrive_near, 0)
    embed_rows(slice(0, near_rows))

    def before_senders(b, carry):
        spot_ = pl.ds(pl.multiple_of(b * batch, batch), batch)
        value = jnp.dot(edge_t[...], embedded[:, spot_], preferred_element_type=f32)
        value = value + jnp.dot(recv_t[...], pick_r[:, spot_], preferred_element_type=f32)
        partial[:, spot_] = value + jnp.dot(
            sender_t[:, 0:near_rows], pick_s[0:near_rows, spot_], preferred_element_type=f32
        )
        return carry

    lax.fori_loop(0, blocks, before_senders, 0)
    msg_t[...] = turned(weight(3)).astype(bf16)
    out_t[...] = turned(weight(4)).astype(bf16)
    node_t[...] = turned(w_node[...].reshape(2 * width, width)).astype(bf16)

    def arrive_far(k, carry):
        for j in range(2):
            @pl.when(k > around)
            def _():
                points(k * 4 + j, me).wait_recv()

            @pl.when(k < half)
            def _():
                points(k * 4 + 2 + j, me).wait_recv()

        return carry

    lax.fori_loop(around, half + 1, arrive_far, 0)
    embed_rows(slice(near_rows, picks))

    def norm(values):
        mean = jnp.mean(values, axis=0, keepdims=True)
        centred = values - mean
        var = jnp.mean(centred * centred, axis=0, keepdims=True)
        return centred * lax.rsqrt(var + norm_eps)

    def add_block(b, carry):
        spot_ = pl.ds(pl.multiple_of(b * batch, batch), batch)
        pre = partial[:, spot_] + jnp.dot(
            sender_t[:, near_rows:], pick_s[near_rows:, spot_], preferred_element_type=f32
        )
        hidden = silu(pre).astype(bf16)
        normed = norm(jnp.dot(msg_t[...], hidden, preferred_element_type=f32))
        message = jnp.concatenate(
            [
                (normed[:, 128 * j : 128 * (j + 1)] * film_b[0] + film_b[1]).astype(bf16)
                for j in range(batch // 128)
            ],
            axis=1,
        )
        total[...] += lax.dot_general(
            message, pick_r[:, spot_], (((1,), (1,)), ((), ())), preferred_element_type=f32
        )
        return carry

    lax.fori_loop(0, blocks, add_block, 0)
    for p in range(3):
        for copy in side_all(p):
            copy.wait_send()

    def sent(e, carry):
        @pl.when(e > 0)
        def _():
            for copy in long_hop(e, z, far_r):
                copy.wait_send()

        for kind in range(3):
            for copy in near(kind, e, z):
                copy.wait_send()

        return carry

    lax.fori_loop(0, 2 * reach, sent, 0)

    for copy in over:
        copy.wait_send()


    def left_(k, carry):
        for j in range(2):
            points(k * 4 + j, me).wait_send()

            @pl.when(k < half)
            def _():
                points(k * 4 + 2 + j, me).wait_send()

        return carry

    points(0, me).wait_send()
    lax.fori_loop(1, half + 1, left_, 0)
    joined[width : 2 * width] = total[...].astype(bf16)
    update = silu(jnp.dot(node_t[...], joined[...], preferred_element_type=f32)).astype(bf16)
    normed = norm(jnp.dot(out_t[...], update, preferred_element_type=f32))
    for j in range(mesh_count // 128):
        lanes = slice(128 * j, 128 * (j + 1))
        value = joined[0:width, lanes].astype(f32) + normed[:, lanes] * film_b[2] + film_b[3]
        out[lanes, :] = value.T.astype(bf16)


def per_device(
    devices, conditioning, target_state, noise_sample, step_index, mesh_features, edge_geometry,
    edge_slot, edge_receiver, send_rows, edge_count, embed_weight, mesh_weight, geom_weight,
    sender_weight, edge_weight, receiver_weight, message_weight, node_weight, output_weight,
    noise_weight, film_weight,
):
    width = embed_weight.shape[1]
    points = conditioning.shape[1]
    chans = (conditioning.shape[0] + target_state.shape[0] + 7) // 8 * 8
    picks = send_rows.size
    slots_n = edge_slot.shape[0]
    mesh_count = mesh_features.shape[1]
    chips = devices // 2
    half = chips // 2
    sem = pltpu.SemaphoreType
    rows, node_rows = sender_weight.shape[0], node_weight.shape[0]
    return pl.pallas_call(
        functools.partial(encoder_kernel, devices),
        out_shape=jax.ShapeDtypeStruct((mesh_count, width), bf16),
        in_specs=[SMEM] * 2 + [VMEM] * 7 + [ANY] * 12,
        out_specs=VMEM,
        scratch_shapes=[
            pltpu.VMEM(conditioning.shape, bf16),
            pltpu.VMEM(target_state.shape, f32),
            pltpu.VMEM(noise_sample.shape, f32),
            pltpu.VMEM(edge_geometry.shape, f32),
            pltpu.VMEM(embed_weight.shape, bf16),
            pltpu.VMEM(film_weight.shape, bf16),
            pltpu.VMEM((chans, points), f32),
            pltpu.VMEM((picks, chans), bf16),
            pltpu.VMEM((picks, chans), bf16),
            pltpu.VMEM((chips, 2, rows, 5 * width), bf16),
            pltpu.VMEM((chips, 2, node_rows, width), bf16),
            pltpu.VMEM((chans, width), f32),
            pltpu.VMEM((8, width), f32),
            pltpu.VMEM((width, slots_n), bf16),
            pltpu.VMEM((picks, slots_n), bf16),
            pltpu.VMEM((mesh_count, slots_n), bf16),
            pltpu.VMEM((width, slots_n), f32),
            pltpu.VMEM((width, picks), bf16),
            pltpu.VMEM((width, mesh_count), bf16),
            pltpu.VMEM((width, width), bf16),
            pltpu.VMEM((width, width), bf16),
            pltpu.VMEM((width, 2 * width), bf16),
            pltpu.VMEM((width, width), bf16),
            pltpu.VMEM((geom_weight.shape[0], width, 128), f32),
            pltpu.VMEM((4, width, 128), f32),
            pltpu.VMEM((2 * width, mesh_count), bf16),
            pltpu.VMEM((width, mesh_count), f32),
            pltpu.VMEM((width, chans), bf16),
            pltpu.VMEM((width, width), bf16),
            sem.DMA((6,)),
            sem.DMA((6,)),
            sem.REGULAR((half + 1,)),
            sem.REGULAR((half + 1,)),
            sem.REGULAR,
            sem.REGULAR,
            sem.DMA((4 * half + 4,)),
            sem.DMA((4 * half + 4,)),
            sem.DMA((2, chips // 4)),
            sem.DMA((2, chips // 4)),
            sem.DMA((3, 2, chips // 4)),
            sem.DMA((3, 2, chips // 4)),
            sem.DMA((3, 2)),
            sem.DMA((3, 2)),
            sem.DMA((2,)),
            sem.DMA((2,)),
        ],
        compiler_params=pltpu.CompilerParams(
            vmem_limit_bytes=LIMIT, collective_id=0, has_side_effects=True
        ),
        name="encoder",
    )(
        step_index, edge_count, send_rows.T, mesh_features, mesh_weight, geom_weight,
        edge_slot.reshape(1, slots_n), edge_receiver.reshape(1, slots_n), noise_weight,
        conditioning, target_state, noise_sample, edge_geometry, embed_weight, film_weight,
        sender_weight, edge_weight, receiver_weight, message_weight, output_weight, node_weight,
    )


def solution(mesh):
    both = P(None, ("member", "node"))
    placed = (
        both, both, both, P("member"), P(None, "node"), P(None, "node"), P("node"), P("node"),
        P("node", None), P("node"), P(), P(), P(), P("node", None), P("node", None), P("node", None),
        P("node", None), P("node", None), P("node", None), P(), P(),
    )
    return jax.shard_map(
        functools.partial(per_device, mesh.shape["node"]),
        mesh=mesh, in_specs=placed, out_specs=P("node", "member"), check_vma=False,
    )
```
